128 devices in a mesh: ctx: 32 (over x, z, core), head: 4 (over y).
Axes of the slice: x: 4, y: 4, z: 4, core: 2. Of those that a mesh axis runs over, the one named last changes fastest.
Arguments:
- query_nope: bfloat16 [32, 16384], P('ctx', 'head'), may hold values from -15 to 15
- query_rope: bfloat16 [32, 8192], P('ctx', 'head'), may hold values from -8 to 8
- cache_latent: bfloat16 [2048, 128, 512], P('ctx'), may hold values from -6 to 6
- cache_rope: bfloat16 [2048, 8192], P('ctx'), may hold values from -8 to 8
- key_up: bfloat16 [128, 128, 512], P('head'), may hold values from -0.25 to 0.25
- value_up: bfloat16 [128, 512, 128], P('head'), may hold values from -0.25 to 0.25
- lengths: int32 [16], replicated, may hold values from 4096 to 16384, as said below
- block_owner: int32 [2048], P('ctx'), may hold values from -1 to 15, as said below
- block_number: int32 [2048], P('ctx'), may hold values from 0 to 127, as said below
Outputs:
- attended: bfloat16 [32, 16384], P('ctx', 'head')
The draws below stay inside these ranges and needn't reach their ends.
Inputs may be any that keep to these rules, and one draw needn't show every extreme that they name: `lengths`: at least one sequence has exactly 16384 positions. A slot with block_owner -1 holds nothing. Sequence b owns exactly ceil(lengths[b] / 128) slots. The slots of sequence b carry block_number 0 to ceil(lengths[b] / 128) - 1, each once; empty slots carry 0.
All inputs are finite; a program needn't handle non-finite values.
Results may differ from the reference program's by a relative error of at most 0.023.
Values may be sent and summed in bfloat16 or wider, within the bound.
A program may use at most 128 MiB of HBM per device.

```python
import math
import jax
import jax.numpy as jnp
from jax import lax

H = 128
NOPE = 128
ROPE = 64
KV_LAT = 512
V_HEAD = 128
SEQS = 16
QT = 2
BLK = 128
NB_DEV = 64
POOL = 2048
ROWS = 32
MAX_LEN = 16384


def pool_layout(key):
    folded = jax.random.fold_in(key, 53)
    splits = jax.random.split(folded, 4)
    shortest = max(QT, MAX_LEN // 4)
    lengths = jax.random.randint(splits[0], (SEQS,), shortest, MAX_LEN + 1, dtype=jnp.int32)
    longest = jax.random.randint(splits[1], (), 0, SEQS, dtype=jnp.int32)
    lengths = jnp.where(jnp.arange(SEQS, dtype=jnp.int32) == longest, MAX_LEN, lengths).astype(jnp.int32)
    needed = (lengths + BLK - 1) // BLK
    block_ends = jnp.cumsum(needed).astype(jnp.int32)
    block_starts = block_ends - needed
    device_count = POOL // NB_DEV
    levels = jax.random.randint(splits[2], (device_count,), 0, 3, dtype=jnp.int32)
    jitter = jax.random.randint(splits[3], (POOL,), 0, 65536, dtype=jnp.int32)
    priority = jnp.repeat(levels, NB_DEV) * 32768 + jitter
    ordering = jnp.argsort(priority, stable=True).astype(jnp.int32)
    ranking = jnp.zeros((POOL,), jnp.int32).at[ordering].set(jnp.arange(POOL, dtype=jnp.int32))
    holder = jnp.sum((ranking[:, None] >= block_ends[None, :]).astype(jnp.int32), axis=1)
    occupied = holder < SEQS
    holder_safe = jnp.minimum(holder, SEQS - 1)
    owners = jnp.where(occupied, holder, -1).astype(jnp.int32)
    numbers = jnp.where(occupied, ranking - block_starts[holder_safe], 0).astype(jnp.int32)
    return (lengths, owners, numbers)


def draw_lengths(key, part):
    return pool_layout(key)[0]


def draw_block_owner(key, part):
    return pool_layout(key)[1]


def draw_block_number(key, part):
    return pool_layout(key)[2]


def draw_query_rope(key, part):
    drawn_key = jax.random.fold_in(key, 31)
    values = jnp.clip(jax.random.normal(drawn_key, (ROWS, H * ROPE), jnp.float32), -8.0, 8.0)
    return values.astype(jnp.bfloat16)


def draw_cache_rope(key, part):
    drawn_key = jax.random.fold_in(key, 41)
    values = jnp.clip(jax.random.normal(drawn_key, (POOL, BLK * ROPE), jnp.float32), -8.0, 8.0)
    return values.astype(jnp.bfloat16)


def block_scale(rng, shape, pieces, least, top_value):
    def one(position, blocks):
        draws = jax.random.uniform(jax.random.fold_in(jax.random.fold_in(rng, 6), position), (blocks,), jnp.float32, least / len(pieces), top_value / len(pieces))
        return jnp.repeat(jnp.exp(draws), shape[position] // blocks).reshape((-1,) + (1,) * (len(shape) - position - 1))

    level = one(*pieces[0])
    for cut in pieces[1:]:
        level = level * one(*cut)
    return level


def noise(own_key, dims, scale, bound, shards=(), held_as=jnp.bfloat16):
    gain = block_scale(own_key, dims, shards, -0.22, 0.18) if shards else 1.0
    result = jax.random.normal(own_key, dims, jnp.float32) * scale * gain
    return jnp.minimum(jnp.maximum(result, -bound), bound).astype(held_as)


def setup_inputs(seed: int = 0) -> dict:
    key_list = jax.random.split(jax.random.key(seed), 10)
    return {
        "query_nope": noise(key_list[0], (ROWS, H * NOPE), 2.5, 15.0, ((0, 32), (1, 4))),
        "query_rope": draw_query_rope(jax.random.fold_in(key_list[9], 71), 0),
        "cache_latent": noise(key_list[2], (POOL, BLK, KV_LAT), 1.0, 6.0, ((0, 32),)),
        "cache_rope": draw_cache_rope(jax.random.fold_in(key_list[9], 71), 0),
        "key_up": noise(key_list[4], (H, NOPE, KV_LAT), KV_LAT ** -0.5, 0.25, ((0, 4),)),
        "value_up": noise(key_list[5], (H, KV_LAT, V_HEAD), KV_LAT ** -0.5, 0.25, ((0, 4),)),
        "lengths": draw_lengths(jax.random.fold_in(key_list[9], 71), 0),
        "block_owner": draw_block_owner(jax.random.fold_in(key_list[9], 71), 0),
        "block_number": draw_block_number(jax.random.fold_in(key_list[9], 71), 0),
    }


score_scale = (192.0 ** -0.5) * (1.0 + 0.1 * math.log(40.0)) ** 2
floor_value = -1.0e30


def reference(query_nope, query_rope, cache_latent, cache_rope, key_up, value_up, lengths, block_owner, block_number):
    query_three = query_nope.reshape(ROWS, H, NOPE).astype(jnp.float32)
    q_latent = jnp.einsum("rhn,hnc->rhc", query_three, key_up.astype(jnp.float32)).astype(jnp.bfloat16)
    q_latent = lax.optimization_barrier(q_latent)
    seq_query = q_latent.reshape(SEQS, QT * H, KV_LAT).astype(jnp.float32)
    seq_rope = query_rope.reshape(SEQS, QT * H, ROPE).astype(jnp.float32)
    per_step = math.gcd(POOL, 64)
    turn_count = POOL // per_step
    latent_sets = cache_latent.reshape(turn_count, per_step, BLK, KV_LAT)
    rope_sets = cache_rope.reshape(turn_count, per_step, BLK, ROPE)
    owner_sets = block_owner.reshape(turn_count, per_step)
    number_sets = block_number.reshape(turn_count, per_step)
    lag_ids = (QT - 1 - jnp.arange(QT)).astype(jnp.int32)
    seq_ids = jnp.arange(SEQS).astype(jnp.int32)
    slot_ids = jnp.arange(BLK).astype(jnp.int32)
    width_q = QT * H

    def advance(running, blockset):
        row_top, row_total, row_accum = running
        key_latent, rope_keys, owners, numbers = blockset
        owner_safe = jnp.clip(owners, 0, SEQS - 1)
        gathered = seq_query[owner_safe]
        gathered_rope = seq_rope[owner_safe]
        latent_real = key_latent.astype(jnp.float32)
        logits = jnp.einsum("gqc,gtc->gqt", gathered, latent_real, precision=lax.Precision.HIGHEST)
        logits = logits + jnp.einsum("gqd,gtd->gqt", gathered_rope, rope_keys.astype(jnp.float32), precision=lax.Precision.HIGHEST)
        logits = logits * score_scale
        positions = numbers[:, None] * BLK + slot_ids[None, :]
        limits = lengths[owner_safe][:, None] - lag_ids[None, :]
        visible = (owners[:, None, None] >= 0) & (positions[:, None, :] < limits[:, :, None])
        visible = jnp.broadcast_to(visible[:, :, None, :], (per_step, QT, H, BLK)).reshape(per_step, width_q, BLK)
        logits = jnp.where(visible, logits, floor_value)
        member = owners[:, None] == seq_ids[None, :]
        block_top = jnp.max(logits, axis=2)
        seq_top = jnp.max(jnp.where(member[:, :, None], block_top[:, None, :], floor_value), axis=0)
        new_top = jnp.maximum(row_top, seq_top)
        weight = jnp.where(visible, jnp.exp(logits - new_top[owner_safe][:, :, None]), 0.0)
        member_real = member.astype(jnp.float32)
        part_total = jnp.einsum("gb,gq->bq", member_real, jnp.sum(weight, axis=2), precision=lax.Precision.HIGHEST)
        weight_low = lax.optimization_barrier(weight.astype(jnp.bfloat16)).astype(jnp.float32)
        values = jnp.einsum("gqt,gtc->gqc", weight_low, latent_real, precision=lax.Precision.HIGHEST)
        part_accum = jnp.einsum("gb,gqc->bqc", member_real, values, precision=lax.Precision.HIGHEST)
        shrink = jnp.exp(row_top - new_top)
        return (new_top, row_total * shrink + part_total, row_accum * shrink[:, :, None] + part_accum), None

    starting = (jnp.full((SEQS, width_q), floor_value, jnp.float32), jnp.zeros((SEQS, width_q), jnp.float32), jnp.zeros((SEQS, width_q, KV_LAT), jnp.float32))
    running, unused = lax.scan(advance, starting, (latent_sets, rope_sets, owner_sets, number_sets))
    latent_out = (running[2] / running[1][:, :, None]).reshape(ROWS, H, KV_LAT)
    attended = jnp.einsum("rhc,hcv->rhv", latent_out, value_up.astype(jnp.float32), precision=lax.Precision.HIGHEST)
    return attended.astype(jnp.bfloat16).reshape(ROWS, H * V_HEAD)
```

```python
import functools
import math

import jax
import jax.numpy as jnp
from jax import lax
from jax.experimental import pallas as pl
from jax.experimental.pallas import tpu as pltpu
from jax.sharding import PartitionSpec as P

MESH = pl.DeviceIdType.MESH
score_scale = 192.0 ** (-0.5) * (1.0 + 0.1 * math.log(40.0)) ** 2
floor_value = -1e30
f32 = jnp.float32
bf16 = jnp.bfloat16
LANES = 128
CORES = 2


def pad8(n):
    return (n + 7) // 8 * 8


class Sizes:
    def __init__(self, ctx, rows, heads, nope, rope, latent, value, slots, block, seqs):
        self.ctx, self.rows, self.heads = ctx, rows, heads
        self.nope, self.rope, self.latent, self.value = nope, rope, latent, value
        self.slots, self.block, self.seqs = slots, block, seqs
        self.chips = ctx // CORES
        self.tokens = rows // seqs
        self.pairs = heads // 2
        self.queries = self.tokens * heads
        self.chunks = latent // LANES
        self.block_rows = heads + self.pairs
        self.gather_stride = pad8(self.block_rows) + 8
        self.head_stride = heads + 8
        self.key_stride = block + 8


def kernel(
    z,
    qn_hbm, qr_hbm, lat_hbm, kr_hbm, ku_hbm, vu_hbm, len_hbm, own_hbm, ownrow_hbm, num_hbm,
    out_ref,
    qn, qr, lat, kr, ku, vu, len_s, own_s, num_s, own_v, meta_v, meta_s,
    gath, qstage, gathf, rk, qlt, ql, qro, sc, mpre, mtop, lpre, opre, ot, yt,
    send, recv, stat, statr, acc,
    load_sem, meta_sem, gs_sem, gr_sem, fs_sem, fr_sem, es_sem, er_sem, ss_sem, sr_sem,
):
    me = lax.axis_index("ctx")
    chip = me // CORES
    core = me - chip * CORES
    partner = chip * CORES + (1 - core)

    def peer_chip(i):
        return lax.rem(chip + i, z.chips)

    def source_chip(i):
        return lax.rem(chip - i + z.chips, z.chips)

    loads = [
        pltpu.make_async_copy(s, d, load_sem.at[k])
        for k, (s, d) in enumerate(
            [(qn_hbm, qn), (qr_hbm, qr), (ownrow_hbm, own_v), (len_hbm, len_s), (own_hbm, own_s),
             (num_hbm, num_s), (kr_hbm, kr), (ku_hbm, ku), (lat_hbm, lat), (vu_hbm, vu)]
        )
    ]
    ld_qn, ld_qr, ld_ownv, ld_len, ld_own, ld_num, ld_kr, ld_ku, ld_lat, ld_vu = loads
    for c in loads:
        c.start()

    barrier = pltpu.get_barrier_semaphore()
    for i in range(z.chips):
        for q in range(CORES):
            target = peer_chip(i) * CORES + lax.rem(core + q, CORES)
            if i == 0 and q == 0:
                continue
            pl.semaphore_signal(barrier, inc=1, device_id={"ctx": target}, device_id_type=MESH)

    ld_qn.wait()
    ld_qr.wait()
    for h in range(z.heads):
        qstage[h : h + 1, :] = qn[:, h * LANES : (h + 1) * LANES].astype(f32)
    for h in range(z.pairs):
        qstage[z.heads + h : z.heads + h + 1, :] = qr[:, h * LANES : (h + 1) * LANES].astype(f32)
    gath[me] = qstage[...].astype(bf16)

    pl.semaphore_wait(barrier, z.ctx - 1)

    def gather_copy(i, row):
        return pltpu.make_async_remote_copy(
            src_ref=gath.at[row], dst_ref=gath.at[row], send_sem=gs_sem.at[i], recv_sem=gr_sem.at[i],
            device_id={"ctx": peer_chip(i) * CORES + core}, device_id_type=MESH,
        )

    def forward_copy(i, row):
        return pltpu.make_async_remote_copy(
            src_ref=gath.at[row], dst_ref=gath.at[row], send_sem=fs_sem.at[i], recv_sem=fr_sem.at[i],
            device_id={"ctx": partner}, device_id_type=MESH,
        )

    order = list(range(1, z.chips))
    for i in order:
        gather_copy(i, me).start()
    forward_copy(0, me).start()

    ld_ownv.wait()
    n = z.slots
    own_row = jnp.broadcast_to(own_v[...], (n, n))
    row_i = lax.broadcasted_iota(jnp.int32, (n, n), 0)
    col_i = lax.broadcasted_iota(jnp.int32, (n, n), 1)
    key_row = own_row * n + col_i
    key_col = jnp.sum(jnp.where(row_i == col_i, key_row, 0), axis=1, keepdims=True)
    rank_col = jnp.sum(jnp.where(key_row < key_col, 1, 0), axis=1, keepdims=True)
    perm = jnp.sum(jnp.where(rank_col == col_i, row_i, 0), axis=0, keepdims=True)
    ends = jnp.sum(jnp.where(key_col < (col_i + 1) * n, 1, 0), axis=0, keepdims=True)
    meta_v[0:1, 0:n] = perm
    meta_v[1:2, 0:n] = ends
    meta_copy = pltpu.make_async_copy(meta_v, meta_s, meta_sem)
    meta_copy.start()

    ld_kr.wait()

    rkf = rk.reshape(n * z.key_stride, LANES)

    def spread_keys(j, carry):
        part = kr[:, pl.ds(pl.multiple_of(j * LANES, LANES), LANES)].astype(f32)
        rkf[pl.ds(2 * j, n, stride=z.key_stride), :] = part
        rkf[pl.ds(2 * j + 1, n, stride=z.key_stride), :] = pltpu.roll(part, z.rope, 1)
        return carry

    lax.fori_loop(0, z.block * z.rope // LANES, spread_keys, 0, unroll=2)

    for i in order:
        gather_copy(i, source_chip(i) * CORES + core).wait_recv()
        forward_copy(i, source_chip(i) * CORES + core).start()
    for i in range(z.chips):
        forward_copy(i, source_chip(i) * CORES + (1 - core)).wait_recv()

    def to_rows(r, carry):
        gathf[pl.ds(pl.multiple_of(r * z.gather_stride, 8), z.block_rows), :] = gath[r].astype(f32)
        return carry

    lax.fori_loop(0, z.rows, to_rows, 0, unroll=2)

    ld_ku.wait()
    span = z.rows * z.head_stride

    def absorb(i, carry):
        for e in range(2):
            h = 2 * i + e
            x = gathf[pl.ds(h, z.rows, stride=z.gather_stride), :].astype(bf16)
            y = jnp.dot(x, ku[h], preferred_element_type=f32)
            place = e * z.pairs + i
            for c in range(z.chunks):
                qlt[pl.ds(c * span + place, z.rows, stride=z.head_stride), :] = y[:, c * LANES : (c + 1) * LANES]
        return carry

    lax.fori_loop(0, z.pairs, absorb, 0, unroll=2)

    lane_p = lax.broadcasted_iota(jnp.int32, (z.pairs, LANES), 1)

    def queries(b, carry):
        for j in range(z.tokens):
            r = b * z.tokens + j
            for c in range(z.chunks):
                start = pl.multiple_of(c * span + r * z.head_stride, 8)
                ql[b, j * z.heads : (j + 1) * z.heads, c * LANES : (c + 1) * LANES] = qlt[
                    pl.ds(start, z.heads), :
                ].astype(bf16)
            both = gathf[pl.ds(pl.multiple_of(r * z.gather_stride + z.heads, 8), z.pairs), :]
            qro[b, j * z.heads : j * z.heads + z.pairs, :] = jnp.where(lane_p < z.rope, both, 0.0)
            other = pltpu.roll(both, z.rope, 1)
            qro[b, j * z.heads + z.pairs : (j + 1) * z.heads, :] = jnp.where(lane_p < z.rope, other, 0.0)
        return carry

    lax.fori_loop(0, z.seqs, queries, 0)

    for c in (ld_len, ld_own, ld_num, ld_lat):
        c.wait()
    meta_copy.wait()
    token = lax.broadcasted_iota(jnp.int32, (z.queries, z.block), 0) // z.heads
    place = lax.broadcasted_iota(jnp.int32, (z.queries, z.block), 1) - token
    contract_last = (((1,), (1,)), ((), ()))

    def score(j, carry):
        top, before = carry
        p = meta_s[0, j]
        o = own_s[p]
        b = jnp.maximum(o, 0)
        limit = jnp.where(o >= 0, len_s[b] - (z.tokens - 1) - num_s[p] * z.block, -z.tokens)
        s = lax.dot_general(ql[b], lat[p], contract_last, preferred_element_type=f32)
        keys = rk[p, 0 : z.block, :]
        s = s + lax.dot_general(qro[b], keys, contract_last, preferred_element_type=f32)
        s = jnp.where(place < limit, s * score_scale, floor_value)
        sc[j] = s
        top = jnp.maximum(jnp.where(o == before, top, floor_value), s)
        mpre[j] = top
        return top, o

    lax.fori_loop(
        0, n, score, (jnp.full((z.queries, z.block), floor_value, f32), jnp.int32(-2)), unroll=4
    )

    lane_q = lax.broadcasted_iota(jnp.int32, (z.queries, LANES), 1)

    def segment(b):
        end = meta_s[1, b]
        return jnp.maximum(end - 1, 0), end

    def has_any(b):
        last, end = segment(b)
        return (end > 0) & (own_s[meta_s[0, last]] == b)

    def tops(b, stats):
        last, _ = segment(b)
        m = jnp.max(mpre[last], axis=1, keepdims=True)
        m = jnp.where(has_any(b), m, floor_value)
        mtop[b] = jnp.broadcast_to(m, (z.queries, z.block))
        return jnp.where(lane_q == b, m, stats)

    stats = lax.fori_loop(0, z.seqs, tops, jnp.zeros((z.queries, LANES), f32), unroll=2)

    def weigh(j, carry):
        total, before = carry
        p = meta_s[0, j]
        o = own_s[p]
        b = jnp.maximum(o, 0)
        w = jnp.exp(sc[j] - mtop[b])
        keep = o == before
        total = jnp.where(keep, total, 0.0) + w
        lpre[j] = total
        old = opre[jnp.maximum(j - 1, 0)]
        opre[j] = jnp.where(keep, old, 0.0) + jnp.dot(w.astype(bf16), lat[p], preferred_element_type=f32)
        return total, o

    lax.fori_loop(0, n, weigh, (jnp.zeros((z.queries, z.block), f32), jnp.int32(-2)), unroll=4)

    def finish(b, stats):
        last, _ = segment(b)
        t = jnp.sum(lpre[last], axis=1, keepdims=True)
        for j in range(z.tokens):
            r = b * z.tokens + j
            for c in range(z.chunks):
                start = pl.multiple_of(c * span + r * z.head_stride, 8)
                ot[pl.ds(start, z.heads), :] = opre[
                    last, j * z.heads : (j + 1) * z.heads, c * LANES : (c + 1) * LANES
                ]
        return jnp.where(lane_q == z.seqs + b, t, stats)

    stats = lax.fori_loop(0, z.seqs, finish, stats)
    turned = jnp.transpose(jnp.concatenate([stats, jnp.zeros((LANES - z.queries, LANES), f32)], axis=0))
    lane_s = lax.broadcasted_iota(jnp.int32, (z.seqs, LANES), 1)
    both = jnp.where(lane_s < LANES // 2, turned[0 : z.seqs], pltpu.roll(turned[z.seqs : 2 * z.seqs], LANES // 2, 1))
    for b in range(z.seqs):
        stat[b] = both[b : b + 1]

    ld_vu.wait()

    def project(i, carry):
        xs = []
        for e in range(2):
            place = e * z.pairs + i
            xs.append(
                jnp.concatenate(
                    [ot[pl.ds(c * span + place, z.rows, stride=z.head_stride), :] for c in range(z.chunks)], axis=1
                )
            )
        x = jnp.concatenate(xs, axis=0).astype(bf16)
        w = jnp.concatenate([vu[2 * i], vu[2 * i + 1]], axis=1)
        y = jnp.dot(x, w, preferred_element_type=f32)
        for e in range(2):
            yt[pl.ds(e * z.pairs + i, z.rows, stride=z.head_stride), :] = y[
                e * z.rows : (e + 1) * z.rows, e * z.value : (e + 1) * z.value
            ]
        return carry

    lax.fori_loop(0, z.pairs, project, 0, unroll=2)

    def packed(r, carry):
        send[r] = yt[pl.ds(pl.multiple_of(r * z.head_stride, 8), z.heads), :].astype(bf16)
        return carry

    lax.fori_loop(0, z.rows, packed, 0, unroll=2)

    def sums_copy(i, q, row, source, sender_core):
        return pltpu.make_async_remote_copy(
            src_ref=send.at[row], dst_ref=recv.at[source], send_sem=es_sem.at[2 * i + q],
            recv_sem=er_sem.at[2 * i + sender_core], device_id={"ctx": row}, device_id_type=MESH,
        )

    def stat_copy(i, q, row, source, sender_core):
        return pltpu.make_async_remote_copy(
            src_ref=stat.at[row // CORES], dst_ref=statr.at[source], send_sem=ss_sem.at[2 * i + q],
            recv_sem=sr_sem.at[2 * i + sender_core], device_id={"ctx": row}, device_id_type=MESH,
        )

    others = [(i, q) for i in range(z.chips) for q in range(CORES) if (i, q) != (0, 0)]

    def target_row(i, q):
        return peer_chip(i) * CORES + (core if q == 0 else 1 - core)

    def source_row(i, q):
        return source_chip(i) * CORES + (core if q == 0 else 1 - core)

    for i, q in others:
        row = target_row(i, q)
        stat_copy(i, q, row, me, q).start()
        sums_copy(i, q, row, me, q).start()
    recv[me] = send[me]
    statr[me] = stat[chip]

    for i, q in others:
        stat_copy(i, q, me, source_row(i, q), q).wait_recv()
        sums_copy(i, q, me, source_row(i, q), q).wait_recv()

    s = jnp.concatenate([statr[d] for d in range(z.ctx)], axis=0)
    s = jnp.where(core == 0, s, pltpu.roll(s, LANES - z.heads, 1))
    t = pltpu.roll(s, LANES // 2, 1)
    top = jnp.max(s, axis=0, keepdims=True)
    factor = jnp.exp(s - top)
    total = jnp.sum(factor * t, axis=0, keepdims=True)
    lane_d = lax.broadcasted_iota(jnp.int32, (z.ctx, LANES), 1)
    share = jnp.where(lane_d < z.heads, factor / jnp.where(lane_d < z.heads, total, 1.0), 0.0)
    share = jnp.transpose(jnp.concatenate([share, jnp.zeros((LANES - z.ctx, LANES), f32)], axis=0))
    merged = jnp.zeros((z.heads, z.value), f32)
    for d in range(z.ctx):
        merged = merged + share[0 : z.heads, d : d + 1] * recv[d].astype(f32)
    acc[...] = merged
    for h in range(z.heads):
        at = (h % 2) * z.pairs + h // 2
        out_ref[:, h * z.value : (h + 1) * z.value] = acc[at : at + 1, :].astype(out_ref.dtype)

    for i in order:
        gather_copy(i, me).wait_send()
    for i in range(z.chips):
        forward_copy(i, source_chip(i) * CORES + core).wait_send()
    for i, q in others:
        row = target_row(i, q)
        stat_copy(i, q, row, me, q).wait_send()
        sums_copy(i, q, row, me, q).wait_send()


def per_device(
    query_nope, query_rope, cache_latent, cache_rope, key_up, value_up, lengths, block_owner, block_number,
):
    ctx = lax.axis_size("ctx")
    heads, nope, latent = key_up.shape
    slots, block, _ = cache_latent.shape
    z = Sizes(
        ctx, query_nope.shape[0] * ctx, heads, nope, query_rope.shape[1] // heads, latent, value_up.shape[2],
        slots, block, lengths.shape[0],
    )
    any_spec = pl.BlockSpec(memory_space=pl.ANY)
    V, S, D = pltpu.VMEM, pltpu.SMEM, pltpu.SemaphoreType.DMA
    span = z.rows * z.head_stride
    scratch = [
        V(query_nope.shape, bf16), V(query_rope.shape, bf16), V(cache_latent.shape, bf16), V(cache_rope.shape, bf16),
        V(key_up.shape, bf16), V(value_up.shape, bf16), S(lengths.shape, jnp.int32), S(block_owner.shape, jnp.int32),
        S(block_number.shape, jnp.int32), V((1, slots), jnp.int32), V((8, LANES), jnp.int32), S((8, LANES), jnp.int32),
        V((z.rows, z.block_rows, LANES), bf16),
        V((z.block_rows, LANES), f32),
        V((z.rows * z.gather_stride, LANES), f32),
        V((slots, z.key_stride, LANES), f32),
        V((z.chunks * span, LANES), f32),
        V((z.seqs, z.queries, latent), bf16),
        V((z.seqs, z.queries, LANES), f32),
        V((slots, z.queries, block), f32),
        V((slots, z.queries, block), f32),
        V((z.seqs, z.queries, block), f32),
        V((slots, z.queries, block), f32),
        V((slots, z.queries, latent), f32),
        V((z.chunks * span, LANES), f32),
        V((span, LANES), f32),
        V((z.rows, heads, z.value), bf16),
        V((z.ctx, heads, z.value), bf16),
        V((z.seqs, 1, LANES), f32),
        V((z.ctx, 1, LANES), f32),
        V((heads, z.value), f32),
        D((10,)), D, D((z.chips,)), D((z.chips,)), D((z.chips,)), D((z.chips,)),
        D((z.ctx,)), D((z.ctx,)), D((z.ctx,)), D((z.ctx,)),
    ]
    return pl.pallas_call(
        functools.partial(kernel, z),
        out_shape=jax.ShapeDtypeStruct((1, heads * z.value), bf16),
        in_specs=[any_spec] * 10,
        out_specs=pl.BlockSpec(memory_space=pltpu.VMEM),
        scratch_shapes=scratch,
        compiler_params=pltpu.CompilerParams(
            collective_id=0, has_side_effects=True, vmem_limit_bytes=64 * 1024 * 1024 - 65536
        ),
    )(
        query_nope, query_rope, cache_latent, cache_rope, key_up, value_up, lengths, block_owner,
        block_owner.reshape(1, slots), block_number,
    )


def solution(mesh):
    return jax.shard_map(
        per_device,
        mesh=mesh,
        in_specs=(
            P("ctx", "head"), P("ctx", "head"), P("ctx", None, None), P("ctx", None), P("head", None, None),
            P("head", None, None), P(), P("ctx"), P("ctx"),
        ),
        out_specs=P("ctx", "head"),
        check_vma=False,
    )
```

```python
import functools
import math

import jax
import jax.numpy as jnp
from jax import lax
from jax.experimental import pallas as pl
from jax.experimental.pallas import tpu as pltpu
from jax.sharding import PartitionSpec as P

MESH = pl.DeviceIdType.MESH
score_scale = 192.0 ** (-0.5) * (1.0 + 0.1 * math.log(40.0)) ** 2
floor_value = -1e30
f32 = jnp.float32
bf16 = jnp.bfloat16
LANES = 128
CORES = 2


def pad8(n):
    return (n + 7) // 8 * 8


class Sizes:
    def __init__(self, ctx, rows, heads, nope, rope, latent, value, slots, block, seqs):
        self.ctx, self.rows, self.heads = ctx, rows, heads
        self.nope, self.rope, self.latent, self.value = nope, rope, latent, value
        self.slots, self.block, self.seqs = slots, block, seqs
        self.chips = ctx // CORES
        self.tokens = rows // seqs
        self.pairs = heads // 2
        self.queries = self.tokens * heads
        self.chunks = latent // LANES
        self.block_rows = heads + self.pairs
        self.gather_stride = pad8(self.block_rows) + 4
        self.head_stride = heads + 4
        self.key_stride = block + 8


def kernel(
    z,
    qn_hbm, qr_hbm, lat_hbm, kr_hbm, ku_hbm, vu_hbm, len_hbm, own_hbm, ownrow_hbm, num_hbm,
    out_ref,
    qn, qr, lat, kr, ku, vu, len_s, own_s, num_s, own_v, meta_v, meta_s,
    gath, qstage, gathf, rk, qlt, ql, qro, sc, mpre, mtop, lpre, opre, ot, yt,
    send, recv, stat, statr, acc,
    load_sem, meta_sem, gs_sem, gr_sem, fs_sem, fr_sem, es_sem, er_sem, ss_sem, sr_sem,
):
    me = lax.axis_index("ctx")
    chip = me // CORES
    core = me - chip * CORES
    partner = chip * CORES + (1 - core)

    side = math.isqrt(z.chips)
    chip_x = chip // side
    chip_z = chip - chip_x * side

    def peer_chip(i):
        return lax.rem(chip_x + i // side, side) * side + lax.rem(chip_z + i % side, side)

    def source_chip(i):
        return lax.rem(chip_x + side - i // side, side) * side + lax.rem(chip_z + side - i % side, side)

    def hops(i):
        return min(i // side, side - i // side) + min(i % side, side - i % side)

    far_first = sorted(range(z.chips), key=lambda i: -hops(i))

    loads = [
        pltpu.make_async_copy(s, d, load_sem.at[k])
        for k, (s, d) in enumerate(
            [(qn_hbm, qn), (qr_hbm, qr), (ownrow_hbm, own_v), (len_hbm, len_s), (own_hbm, own_s),
             (num_hbm, num_s), (kr_hbm, kr), (ku_hbm, ku), (lat_hbm, lat), (vu_hbm, vu)]
        )
    ]
    ld_qn, ld_qr, ld_ownv, ld_len, ld_own, ld_num, ld_kr, ld_ku, ld_lat, ld_vu = loads
    for c in loads:
        c.start()

    barrier = pltpu.get_barrier_semaphore()
    for i in range(z.chips):
        for q in range(CORES):
            target = peer_chip(i) * CORES + lax.rem(core + q, CORES)
            if i == 0 and q == 0:
                continue
            pl.semaphore_signal(barrier, inc=1, device_id={"ctx": target}, device_id_type=MESH)

    ld_qn.wait()
    ld_qr.wait()
    for h in range(z.heads):
        qstage[h : h + 1, :] = qn[:, h * LANES : (h + 1) * LANES].astype(f32)
    for h in range(z.pairs):
        qstage[z.heads + h : z.heads + h + 1, :] = qr[:, h * LANES : (h + 1) * LANES].astype(f32)
    gath[me] = qstage[...].astype(bf16)

    pl.semaphore_wait(barrier, z.ctx - 1)

    def gather_copy(i, row):
        return pltpu.make_async_remote_copy(
            src_ref=gath.at[row], dst_ref=gath.at[row], send_sem=gs_sem.at[i], recv_sem=gr_sem.at[i],
            device_id={"ctx": peer_chip(i) * CORES + core}, device_id_type=MESH,
        )

    def forward_copy(i, row):
        return pltpu.make_async_remote_copy(
            src_ref=gath.at[row], dst_ref=gath.at[row], send_sem=fs_sem.at[i], recv_sem=fr_sem.at[i],
            device_id={"ctx": partner}, device_id_type=MESH,
        )

    order = [i for i in far_first if i]
    for i in order:
        gather_copy(i, me).start()
    forward_copy(0, me).start()

    ld_ownv.wait()
    n = z.slots
    own_row = jnp.broadcast_to(own_v[...], (n, n))
    row_i = lax.broadcasted_iota(jnp.int32, (n, n), 0)
    col_i = lax.broadcasted_iota(jnp.int32, (n, n), 1)
    key_row = own_row * n + col_i
    key_col = jnp.sum(jnp.where(row_i == col_i, key_row, 0), axis=1, keepdims=True)
    rank_col = jnp.sum(jnp.where(key_row < key_col, 1, 0), axis=1, keepdims=True)
    perm = jnp.sum(jnp.where(rank_col == col_i, row_i, 0), axis=0, keepdims=True)
    ends = jnp.sum(jnp.where(key_col < (col_i + 1) * n, 1, 0), axis=0, keepdims=True)
    meta_v[0:1, 0:n] = perm
    meta_v[1:2, 0:n] = ends
    meta_copy = pltpu.make_async_copy(meta_v, meta_s, meta_sem)
    meta_copy.start()

    ld_kr.wait()

    rkf = rk.reshape(n * z.key_stride, LANES)

    def spread_keys(j, carry):
        part = kr[:, pl.ds(pl.multiple_of(j * LANES, LANES), LANES)].astype(f32)
        rkf[pl.ds(2 * j, n, stride=z.key_stride), :] = part
        rkf[pl.ds(2 * j + 1, n, stride=z.key_stride), :] = pltpu.roll(part, z.rope, 1)
        return carry

    lax.fori_loop(0, z.block * z.rope // LANES, spread_keys, 0, unroll=4)

    for i in order[::-1]:
        gather_copy(i, source_chip(i) * CORES + core).wait_recv()
        forward_copy(i, source_chip(i) * CORES + core).start()
    for i in range(z.chips):
        forward_copy(i, source_chip(i) * CORES + (1 - core)).wait_recv()

    def to_rows(r, carry):
        gathf[pl.ds(r * z.gather_stride, z.block_rows), :] = gath[r].astype(f32)
        return carry

    lax.fori_loop(0, z.rows, to_rows, 0, unroll=2)

    ld_ku.wait()
    span = z.rows * z.head_stride

    def absorb(i, carry):
        for e in range(2):
            h = 2 * i + e
            x = gathf[pl.ds(h, z.rows, stride=z.gather_stride), :].astype(bf16)
            y = jnp.dot(x, ku[h], preferred_element_type=f32)
            place = e * z.pairs + i
            for c in range(z.chunks):
                qlt[pl.ds(c * span + place, z.rows, stride=z.head_stride), :] = y[:, c * LANES : (c + 1) * LANES]
        return carry

    lax.fori_loop(0, z.pairs, absorb, 0, unroll=8)

    lane_p = lax.broadcasted_iota(jnp.int32, (z.pairs, LANES), 1)

    def queries(b, carry):
        for j in range(z.tokens):
            r = b * z.tokens + j
            for c in range(z.chunks):
                start = c * span + r * z.head_stride
                ql[b, j * z.heads : (j + 1) * z.heads, c * LANES : (c + 1) * LANES] = qlt[
                    pl.ds(start, z.heads), :
                ].astype(bf16)
            both = gathf[pl.ds(r * z.gather_stride + z.heads, z.pairs), :]
            qro[b, j * z.heads : j * z.heads + z.pairs, :] = jnp.where(lane_p < z.rope, both, 0.0)
            other = pltpu.roll(both, z.rope, 1)
            qro[b, j * z.heads + z.pairs : (j + 1) * z.heads, :] = jnp.where(lane_p < z.rope, other, 0.0)
        return carry

    lax.fori_loop(0, z.seqs, queries, 0, unroll=4)

    for c in (ld_len, ld_own, ld_num, ld_lat):
        c.wait()
    meta_copy.wait()
    token = lax.broadcasted_iota(jnp.int32, (z.queries, z.block), 0) // z.heads
    place = lax.broadcasted_iota(jnp.int32, (z.queries, z.block), 1) - token
    contract_last = (((1,), (1,)), ((), ()))

    def score(g, carry):
        top, before = carry
        js = [2 * g, 2 * g + 1]
        ps = [meta_s[0, j] for j in js]
        os = [own_s[p] for p in ps]
        bs = [jnp.maximum(o, 0) for o in os]
        lhs = jnp.concatenate([ql[b] for b in bs], axis=0)
        rhs = jnp.concatenate([lat[p] for p in ps], axis=0)
        full = lax.dot_general(lhs, rhs, contract_last, preferred_element_type=f32)
        lhs = jnp.concatenate([qro[b] for b in bs], axis=0)
        rhs = jnp.concatenate([rk[p, 0 : z.block, :] for p in ps], axis=0)
        full = full + lax.dot_general(lhs, rhs, contract_last, preferred_element_type=f32)
        for u in range(2):
            p, o, j = ps[u], os[u], js[u]
            limit = jnp.where(o >= 0, len_s[bs[u]] - (z.tokens - 1) - num_s[p] * z.block, -z.tokens)
            s = full[u * z.queries : (u + 1) * z.queries, u * z.block : (u + 1) * z.block]
            s = jnp.where(place < limit, s * score_scale, floor_value)
            sc[j] = s
            top = jnp.maximum(jnp.where(o == before, top, floor_value), s)
            mpre[j] = top
            before = o
        return top, before

    lax.fori_loop(
        0, n // 2, score, (jnp.full((z.queries, z.block), floor_value, f32), jnp.int32(-2)), unroll=8
    )

    lane_q = lax.broadcasted_iota(jnp.int32, (z.queries, LANES), 1)

    def segment(b):
        end = meta_s[1, b]
        return jnp.maximum(end - 1, 0), end

    def has_any(b):
        last, end = segment(b)
        return (end > 0) & (own_s[meta_s[0, last]] == b)

    def tops(b, stats):
        last, _ = segment(b)
        m = jnp.max(mpre[last], axis=1, keepdims=True)
        m = jnp.where(has_any(b), m, floor_value)
        mtop[b] = jnp.broadcast_to(m, (z.queries, z.block))
        return jnp.where(lane_q == b, m, stats)

    stats = lax.fori_loop(0, z.seqs, tops, jnp.zeros((z.queries, LANES), f32), unroll=4)

    def weigh(j, carry):
        total, run, before = carry
        p = meta_s[0, j]
        o = own_s[p]
        b = jnp.maximum(o, 0)
        w = jnp.exp(sc[j] - mtop[b])
        keep = o == before
        total = jnp.where(keep, total, 0.0) + w
        lpre[j] = total
        run = jnp.where(keep, run, 0.0) + jnp.dot(w.astype(bf16), lat[p], preferred_element_type=f32)
        opre[j] = run
        return total, run, o

    lax.fori_loop(0, n, weigh, (jnp.zeros((z.queries, z.block), f32), jnp.zeros((z.queries, z.latent), f32), jnp.int32(-2)), unroll=16)

    def finish(b, stats):
        last, _ = segment(b)
        t = jnp.sum(lpre[last], axis=1, keepdims=True)
        for j in range(z.tokens):
            r = b * z.tokens + j
            for c in range(z.chunks):
                start = c * span + r * z.head_stride
                ot[pl.ds(start, z.heads), :] = opre[
                    last, j * z.heads : (j + 1) * z.heads, c * LANES : (c + 1) * LANES
                ]
        return jnp.where(lane_q == z.seqs + b, t, stats)

    stats = lax.fori_loop(0, z.seqs, finish, stats, unroll=4)
    turned = jnp.transpose(jnp.concatenate([stats, jnp.zeros((LANES - z.queries, LANES), f32)], axis=0))
    lane_s = lax.broadcasted_iota(jnp.int32, (z.seqs, LANES), 1)
    both = jnp.where(lane_s < LANES // 2, turned[0 : z.seqs], pltpu.roll(turned[z.seqs : 2 * z.seqs], LANES // 2, 1))
    for b in range(z.seqs):
        stat[b] = both[b : b + 1]

    ld_vu.wait()

    def project(i, carry):
        xs = []
        for e in range(2):
            place = e * z.pairs + i
            xs.append(
                jnp.concatenate(
                    [ot[pl.ds(c * span + place, z.rows, stride=z.head_stride), :] for c in range(z.chunks)], axis=1
                )
            )
        x = jnp.concatenate(xs, axis=0).astype(bf16)
        w = jnp.concatenate([vu[2 * i], vu[2 * i + 1]], axis=1)
        y = jnp.dot(x, w, preferred_element_type=f32)
        for e in range(2):
            yt[pl.ds(e * z.pairs + i, z.rows, stride=z.head_stride), :] = y[
                e * z.rows : (e + 1) * z.rows, e * z.value : (e + 1) * z.value
            ]
        return carry

    lax.fori_loop(0, z.pairs, project, 0, unroll=8)

    def packed(r, carry):
        send[r] = yt[pl.ds(r * z.head_stride, z.heads), :].astype(bf16)
        return carry

    lax.fori_loop(0, z.rows, packed, 0, unroll=2)

    def sums_copy(i, q, row, source, sender_core):
        return pltpu.make_async_remote_copy(
            src_ref=send.at[row], dst_ref=recv.at[source], send_sem=es_sem.at[2 * i + q],
            recv_sem=er_sem.at[2 * i + sender_core], device_id={"ctx": row}, device_id_type=MESH,
        )

    def stat_copy(i, q, row, source, sender_core):
        return pltpu.make_async_remote_copy(
            src_ref=stat.at[row // CORES], dst_ref=statr.at[source], send_sem=ss_sem.at[2 * i + q],
            recv_sem=sr_sem.at[2 * i + sender_core], device_id={"ctx": row}, device_id_type=MESH,
        )

    others = [(i, q) for i in far_first for q in range(CORES) if (i, q) != (0, 0)]

    def target_row(i, q):
        return peer_chip(i) * CORES + (core if q == 0 else 1 - core)

    def source_row(i, q):
        return source_chip(i) * CORES + (core if q == 0 else 1 - core)

    for i, q in others:
        row = target_row(i, q)
        stat_copy(i, q, row, me, q).start()
        sums_copy(i, q, row, me, q).start()
    recv[me] = send[me]
    statr[me] = stat[chip]

    for i, q in others:
        stat_copy(i, q, me, source_row(i, q), q).wait_recv()
        sums_copy(i, q, me, source_row(i, q), q).wait_recv()

    s = jnp.concatenate([statr[d] for d in range(z.ctx)], axis=0)
    s = jnp.where(core == 0, s, pltpu.roll(s, LANES - z.heads, 1))
    t = pltpu.roll(s, LANES // 2, 1)
    top = jnp.max(s, axis=0, keepdims=True)
    factor = jnp.exp(s - top)
    total = jnp.sum(factor * t, axis=0, keepdims=True)
    lane_d = lax.broadcasted_iota(jnp.int32, (z.ctx, LANES), 1)
    share = jnp.where(lane_d < z.heads, factor / jnp.where(lane_d < z.heads, total, 1.0), 0.0)
    share = jnp.transpose(jnp.concatenate([share, jnp.zeros((LANES - z.ctx, LANES), f32)], axis=0))
    merged = jnp.zeros((z.heads, z.value), f32)
    for d in range(z.ctx):
        merged = merged + share[0 : z.heads, d : d + 1] * recv[d].astype(f32)
    acc[...] = merged
    for h in range(z.heads):
        at = (h % 2) * z.pairs + h // 2
        out_ref[:, h * z.value : (h + 1) * z.value] = acc[at : at + 1, :].astype(out_ref.dtype)

    for i in order:
        gather_copy(i, me).wait_send()
    for i in range(z.chips):
        forward_copy(i, source_chip(i) * CORES + core).wait_send()
    for i, q in others:
        row = target_row(i, q)
        stat_copy(i, q, row, me, q).wait_send()
        sums_copy(i, q, row, me, q).wait_send()


def per_device(
    query_nope, query_rope, cache_latent, cache_rope, key_up, value_up, lengths, block_owner, block_number,
):
    ctx = lax.axis_size("ctx")
    heads, nope, latent = key_up.shape
    slots, block, _ = cache_latent.shape
    z = Sizes(
        ctx, query_nope.shape[0] * ctx, heads, nope, query_rope.shape[1] // heads, latent, value_up.shape[2],
        slots, block, lengths.shape[0],
    )
    any_spec = pl.BlockSpec(memory_space=pl.ANY)
    V, S, D = pltpu.VMEM, pltpu.SMEM, pltpu.SemaphoreType.DMA
    span = z.rows * z.head_stride
    scratch = [
        V(query_nope.shape, bf16), V(query_rope.shape, bf16), V(cache_latent.shape, bf16), V(cache_rope.shape, bf16),
        V(key_up.shape, bf16), V(value_up.shape, bf16), S(lengths.shape, jnp.int32), S(block_owner.shape, jnp.int32),
        S(block_number.shape, jnp.int32), V((1, slots), jnp.int32), V((8, LANES), jnp.int32), S((8, LANES), jnp.int32),
        V((z.rows, z.block_rows, LANES), bf16),
        V((z.block_rows, LANES), f32),
        V((z.rows * z.gather_stride, LANES), f32),
        V((slots, z.key_stride, LANES), f32),
        V((z.chunks * span, LANES), f32),
        V((z.seqs, z.queries, latent), bf16),
        V((z.seqs, z.queries, LANES), f32),
        V((slots, z.queries, block), f32),
        V((slots, z.queries, block), f32),
        V((z.seqs, z.queries, block), f32),
        V((slots, z.queries, block), f32),
        V((slots, z.queries, latent), f32),
        V((z.chunks * span, LANES), f32),
        V((span, LANES), f32),
        V((z.rows, heads, z.value), bf16),
        V((z.ctx, heads, z.value), bf16),
        V((z.seqs, 1, LANES), f32),
        V((z.ctx, 1, LANES), f32),
        V((heads, z.value), f32),
        D((10,)), D, D((z.chips,)), D((z.chips,)), D((z.chips,)), D((z.chips,)),
        D((z.ctx,)), D((z.ctx,)), D((z.ctx,)), D((z.ctx,)),
    ]
    return pl.pallas_call(
        functools.partial(kernel, z),
        out_shape=jax.ShapeDtypeStruct((1, heads * z.value), bf16),
        in_specs=[any_spec] * 10,
        out_specs=pl.BlockSpec(memory_space=pltpu.VMEM),
        scratch_shapes=scratch,
        compiler_params=pltpu.CompilerParams(
            collective_id=0, has_side_effects=True, vmem_limit_bytes=64 * 1024 * 1024 - 65536
        ),
    )(
        query_nope, query_rope, cache_latent, cache_rope, key_up, value_up, lengths, block_owner,
        block_owner.reshape(1, slots), block_number,
    )


def solution(mesh):
    return jax.shard_map(
        per_device,
        mesh=mesh,
        in_specs=(
            P("ctx", "head"), P("ctx", "head"), P("ctx", None, None), P("ctx", None), P("head", None, None),
            P("head", None, None), P(), P("ctx"), P("ctx"),
        ),
        out_specs=P("ctx", "head"),
        check_vma=False,
    )
```

```python
import functools
import math

import jax
import jax.numpy as jnp
from jax import lax
from jax.experimental import pallas as pl
from jax.experimental.pallas import tpu as pltpu
from jax.sharding import PartitionSpec as P

MESH = pl.DeviceIdType.MESH
score_scale = 192.0 ** (-0.5) * (1.0 + 0.1 * math.log(40.0)) ** 2
floor_value = -1e30
f32 = jnp.float32
bf16 = jnp.bfloat16
LANES = 128
CORES = 2


def pad8(n):
    return (n + 7) // 8 * 8


class Sizes:
    def __init__(self, ctx, rows, heads, nope, rope, latent, value, slots, block, seqs):
        self.ctx, self.rows, self.heads = ctx, rows, heads
        self.nope, self.rope, self.latent, self.value = nope, rope, latent, value
        self.slots, self.block, self.seqs = slots, block, seqs
        self.chips = ctx // CORES
        self.tokens = rows // seqs
        self.pairs = heads // 2
        self.queries = self.tokens * heads
        self.chunks = latent // LANES
        self.block_rows = heads + self.pairs
        self.gather_stride = pad8(self.block_rows) + 4
        self.head_stride = heads + 4
        self.key_stride = block + 8


def kernel(
    z,
    qn_hbm, qr_hbm, lat_hbm, kr_hbm, ku_hbm, vu_hbm, len_hbm, own_hbm, ownrow_hbm, num_hbm,
    out_ref,
    qn, qr, lat, kr, ku, vu, len_s, own_s, num_s, own_v, meta_v, meta_s,
    gath, qstage, gathf, rk, kt, qlt, ql, qro, sc, mpre, mtop, mpart, lpre, opre, ot, yt,
    sendp, part, send, recv, stat, statp, statf, statr, acc,
    load_sem, meta_sem, ready, gs_sem, gr_sem, fs_sem, fr_sem, bs_sem, br_sem, fbs_sem, fbr_sem, ps_sem, pr_sem, es_sem, er_sem, ss_sem, sr_sem,
):
    me = lax.axis_index("ctx")
    chip = me // CORES
    core = me - chip * CORES
    partner = chip * CORES + (1 - core)

    side = math.isqrt(z.chips)
    chip_x = chip // side
    chip_z = chip - chip_x * side

    def peer_chip(i):
        return lax.rem(chip_x + i // side, side) * side + lax.rem(chip_z + i % side, side)

    def source_chip(i):
        return lax.rem(chip_x + side - i // side, side) * side + lax.rem(chip_z + side - i % side, side)

    def hops(i):
        return min(i // side, side - i // side) + min(i % side, side - i % side)

    def layer(dz):
        return lax.rem(chip_z + dz, side)

    def source_layer(dz):
        return lax.rem(chip_z + side - dz, side)

    def on_layer(dz, test, act):
        if dz:
            pl.when(test(layer(dz)))(act)
        else:
            act()

    def from_layer(dz, test, act):
        pl.when(test(source_layer(dz)))(act)

    far_first = sorted(range(z.chips), key=lambda i: -hops(i))

    loads = [
        pltpu.make_async_copy(s, d, load_sem.at[k])
        for k, (s, d) in enumerate(
            [(qn_hbm, qn), (qr_hbm, qr), (ownrow_hbm, own_v), (len_hbm, len_s), (own_hbm, own_s),
             (num_hbm, num_s), (kr_hbm, kr), (ku_hbm, ku), (lat_hbm, lat), (vu_hbm, vu)]
        )
    ]
    ld_qn, ld_qr, ld_ownv, ld_len, ld_own, ld_num, ld_kr, ld_ku, ld_lat, ld_vu = loads
    for c in loads:
        c.start()

    barrier = pltpu.get_barrier_semaphore()
    for i in range(z.chips):
        target = peer_chip(i) * CORES + core if i else partner

        def greet():
            pl.semaphore_signal(barrier, inc=1, device_id={"ctx": target}, device_id_type=MESH)

        on_layer(i % side, lambda there: there > chip_z, greet)

    ld_qn.wait()
    ld_qr.wait()
    for h in range(z.heads):
        qstage[h : h + 1, :] = qn[:, h * LANES : (h + 1) * LANES].astype(f32)
    for h in range(z.pairs):
        qstage[z.heads + h : z.heads + h + 1, :] = qr[:, h * LANES : (h + 1) * LANES].astype(f32)
    own_slot = core * z.chips + chip_z * side + chip_x
    gath[own_slot] = qstage[...].astype(bf16)

    pl.semaphore_wait(barrier, side + side * chip_z)

    def slot_of(i, which):
        return which * z.chips + source_layer(i % side) * side + lax.rem(chip_x + side - i // side, side)

    def gather_copy(i, slot):
        return pltpu.make_async_remote_copy(
            src_ref=gath.at[slot], dst_ref=gath.at[slot], send_sem=gs_sem.at[i], recv_sem=gr_sem.at[i],
            device_id={"ctx": peer_chip(i) * CORES + core}, device_id_type=MESH,
        )

    def forward_copy(i, which):
        return pltpu.make_async_remote_copy(
            src_ref=gath.at[slot_of(i, which)], dst_ref=gath.at[slot_of(i, which)], send_sem=fs_sem.at[i],
            recv_sem=fr_sem.at[i], device_id={"ctx": partner}, device_id_type=MESH,
        )

    def layer_rows(at, which):
        return gath.at[pl.ds(which * z.chips + at * side, side)]

    def layer_copy(dz, at):
        return pltpu.make_async_remote_copy(
            src_ref=layer_rows(at, core), dst_ref=layer_rows(at, core), send_sem=bs_sem.at[dz], recv_sem=br_sem.at[dz],
            device_id={"ctx": (chip_x * side + layer(dz)) * CORES + core}, device_id_type=MESH,
        )

    def forward_layer(dz, which):
        rows = layer_rows(source_layer(dz), which)
        return pltpu.make_async_remote_copy(
            src_ref=rows, dst_ref=rows, send_sem=fbs_sem.at[dz], recv_sem=fbr_sem.at[dz],
            device_id={"ctx": partner}, device_id_type=MESH,
        )

    order = [i for i in far_first if i]
    level = [i for i in order if i % side == 0]
    layers = range(1, side)

    def lower(there):
        return there < chip_z

    def higher(there):
        return there > chip_z

    for dz in layers:

        def tell():
            pl.semaphore_signal(
                ready.at[side - dz], inc=1, device_id={"ctx": (chip_x * side + layer(dz)) * CORES + core}, device_id_type=MESH
            )

        on_layer(dz, lower, tell)
    for i in order:
        on_layer(i % side, lower, lambda: gather_copy(i, own_slot).start())
    forward_copy(0, core).start()

    ld_ownv.wait()
    n = z.slots
    own_row = jnp.broadcast_to(own_v[...], (n, n))
    row_i = lax.broadcasted_iota(jnp.int32, (n, n), 0)
    col_i = lax.broadcasted_iota(jnp.int32, (n, n), 1)
    key_row = own_row * n + col_i
    key_col = jnp.sum(jnp.where(row_i == col_i, key_row, 0), axis=1, keepdims=True)
    rank_col = jnp.sum(jnp.where(key_row < key_col, 1, 0), axis=1, keepdims=True)
    perm = jnp.sum(jnp.where(rank_col == col_i, row_i, 0), axis=0, keepdims=True)
    ends = jnp.sum(jnp.where(key_col < (col_i + 1) * n, 1, 0), axis=0, keepdims=True)
    meta_v[0:1, 0:n] = perm
    meta_v[1:2, 0:n] = ends
    meta_copy = pltpu.make_async_copy(meta_v, meta_s, meta_sem)
    meta_copy.start()

    ld_kr.wait()

    rkf = rk.reshape(n * z.key_stride, LANES)

    def spread_keys(j, carry):
        part = kr[:, pl.ds(pl.multiple_of(j * LANES, LANES), LANES)].astype(f32)
        rkf[pl.ds(2 * j, n, stride=z.key_stride), :] = part
        rkf[pl.ds(2 * j + 1, n, stride=z.key_stride), :] = pltpu.roll(part, z.rope, 1)
        return carry

    lax.fori_loop(0, z.block * z.rope // LANES, spread_keys, 0, unroll=4)

    def turn_keys(p, carry):
        kt[p] = jnp.transpose(lat[p])
        return carry

    ld_lat.wait()
    lax.fori_loop(0, n // 2, turn_keys, 0, unroll=2)

    for i in level:
        gather_copy(i, slot_of(i, core)).wait_recv()
        forward_copy(i, core).start()
    for dz in layers:

        def hand_on():
            pl.semaphore_wait(ready.at[dz], 1)
            layer_copy(dz, chip_z).start()

        on_layer(dz, higher, hand_on)

    lax.fori_loop(n // 2, n - n // 4, turn_keys, 0, unroll=2)

    for dz in layers:

        def from_lower():
            layer_copy(dz, source_layer(dz)).wait_recv()
            forward_layer(dz, core).start()

        def from_higher():
            for i in order:
                if i % side == dz:
                    gather_copy(i, slot_of(i, core)).wait_recv()
                    forward_copy(i, core).start()

        from_layer(dz, lower, from_lower)
        from_layer(dz, higher, from_higher)

    lax.fori_loop(n - n // 4, n, turn_keys, 0, unroll=2)

    forward_copy(0, 1 - core).wait_recv()
    for i in level:
        forward_copy(i, 1 - core).wait_recv()
    for dz in layers:

        def part_of_lower():
            forward_layer(dz, 1 - core).wait_recv()

        def part_of_higher():
            for i in order:
                if i % side == dz:
                    forward_copy(i, 1 - core).wait_recv()

        from_layer(dz, lower, part_of_lower)
        from_layer(dz, higher, part_of_higher)

    for chip_of in range(z.chips):
        for which in range(CORES):
            slot = which * z.chips + chip_of % side * side + chip_of // side
            gathf[pl.ds((chip_of * CORES + which) * z.gather_stride, z.block_rows), :] = gath[slot].astype(f32)

    ld_ku.wait()
    span = z.rows * z.head_stride

    def absorb(i, carry):
        for e in range(2):
            h = 2 * i + e
            x = gathf[pl.ds(h, z.rows, stride=z.gather_stride), :].astype(bf16)
            y = jnp.dot(x, ku[h], preferred_element_type=f32)
            place = e * z.pairs + i
            for c in range(z.chunks):
                qlt[pl.ds(c * span + place, z.rows, stride=z.head_stride), :] = y[:, c * LANES : (c + 1) * LANES]
        return carry

    lax.fori_loop(0, z.pairs, absorb, 0, unroll=8)

    lane_p = lax.broadcasted_iota(jnp.int32, (z.pairs, LANES), 1)

    def queries(b, carry):
        for j in range(z.tokens):
            r = b * z.tokens + j
            for c in range(z.chunks):
                start = c * span + r * z.head_stride
                ql[b, j * z.heads : (j + 1) * z.heads, c * LANES : (c + 1) * LANES] = qlt[
                    pl.ds(start, z.heads), :
                ].astype(bf16)
            both = gathf[pl.ds(r * z.gather_stride + z.heads, z.pairs), :]
            qro[b, j * z.heads : j * z.heads + z.pairs, :] = jnp.where(lane_p < z.rope, both, 0.0)
            other = pltpu.roll(both, z.rope, 1)
            qro[b, j * z.heads + z.pairs : (j + 1) * z.heads, :] = jnp.where(lane_p < z.rope, other, 0.0)
        return carry

    lax.fori_loop(0, z.seqs, queries, 0, unroll=4)

    for c in (ld_len, ld_own, ld_num):
        c.wait()
    meta_copy.wait()
    token = lax.broadcasted_iota(jnp.int32, (z.queries, z.block), 0) // z.heads
    place = lax.broadcasted_iota(jnp.int32, (z.queries, z.block), 1) - token
    contract_last = (((1,), (1,)), ((), ()))

    def score(g, carry):
        top, before = carry
        js = [2 * g, 2 * g + 1]
        ps = [meta_s[0, j] for j in js]
        os = [own_s[p] for p in ps]
        bs = [jnp.maximum(o, 0) for o in os]
        lhs = jnp.concatenate([ql[b] for b in bs], axis=0)
        rhs = jnp.concatenate([kt[p] for p in ps], axis=1)
        full = jnp.dot(lhs, rhs, preferred_element_type=f32)
        lhs = jnp.concatenate([qro[b] for b in bs], axis=0)
        rhs = jnp.concatenate([rk[p, 0 : z.block, :] for p in ps], axis=0)
        full = full + lax.dot_general(lhs, rhs, contract_last, preferred_element_type=f32)
        for u in range(2):
            p, o, j = ps[u], os[u], js[u]
            limit = jnp.where(o >= 0, len_s[bs[u]] - (z.tokens - 1) - num_s[p] * z.block, -z.tokens)
            s = full[u * z.queries : (u + 1) * z.queries, u * z.block : (u + 1) * z.block]
            s = jnp.where(place < limit, s * score_scale, floor_value)
            sc[j] = s
            top = jnp.maximum(jnp.where(o == before, top, floor_value), s)
            mpre[j] = top
            before = o
        return top, before

    lax.fori_loop(
        0, n // 2, score, (jnp.full((z.queries, z.block), floor_value, f32), jnp.int32(-2)), unroll=8
    )

    lane_q = lax.broadcasted_iota(jnp.int32, (z.queries, LANES), 1)

    def segment(b):
        end = meta_s[1, b]
        return jnp.maximum(end - 1, 0), end

    def has_any(b):
        last, end = segment(b)
        return (end > 0) & (own_s[meta_s[0, last]] == b)

    def tops(b, carry):
        last, _ = segment(b)
        m = jnp.max(mpre[last], axis=1, keepdims=True)
        mtop[b] = jnp.broadcast_to(jnp.where(has_any(b), m, floor_value), (z.queries, z.block))
        return carry

    lax.fori_loop(0, z.seqs, tops, 0, unroll=4)

    def pair_copy(k, src, dst):
        return pltpu.make_async_remote_copy(
            src_ref=src, dst_ref=dst, send_sem=ps_sem.at[k], recv_sem=pr_sem.at[k],
            device_id={"ctx": partner}, device_id_type=MESH,
        )

    top_copy = pair_copy(0, mtop, mpart)
    top_copy.start()

    def weigh(j, carry):
        total, run, before = carry
        p = meta_s[0, j]
        o = own_s[p]
        b = jnp.maximum(o, 0)
        w = jnp.exp(sc[j] - mtop[b])
        keep = o == before
        total = jnp.where(keep, total, 0.0) + w
        lpre[j] = total
        run = jnp.where(keep, run, 0.0) + jnp.dot(w.astype(bf16), lat[p], preferred_element_type=f32)
        opre[j] = run
        return total, run, o

    lax.fori_loop(0, n, weigh, (jnp.zeros((z.queries, z.block), f32), jnp.zeros((z.queries, z.latent), f32), jnp.int32(-2)), unroll=16)

    top_copy.wait_recv()

    def finish(b, stats):
        last, _ = segment(b)
        mine = mtop[b]
        pair = jnp.maximum(mine, mpart[b])
        scale = jnp.exp(mine - pair)
        t = jnp.sum(lpre[last] * scale, axis=1, keepdims=True)
        for j in range(z.tokens):
            r = b * z.tokens + j
            for c in range(z.chunks):
                start = c * span + r * z.head_stride
                ot[pl.ds(start, z.heads), :] = (
                    opre[last, j * z.heads : (j + 1) * z.heads, c * LANES : (c + 1) * LANES]
                    * scale[j * z.heads : (j + 1) * z.heads]
                )
        stats = jnp.where(lane_q == b, pair, stats)
        return jnp.where(lane_q == z.seqs + b, t, stats)

    stats = lax.fori_loop(0, z.seqs, finish, jnp.zeros((z.queries, LANES), f32), unroll=4)
    turned = jnp.transpose(jnp.concatenate([stats, jnp.zeros((LANES - z.queries, LANES), f32)], axis=0))
    lane_s = lax.broadcasted_iota(jnp.int32, (z.seqs, LANES), 1)
    stat[...] = jnp.where(
        lane_s < LANES // 2, turned[0 : z.seqs], pltpu.roll(turned[z.seqs : 2 * z.seqs], LANES // 2, 1)
    )
    stat_pair = pair_copy(1, stat, statp)
    stat_pair.start()

    ld_vu.wait()
    group = z.pairs // 2

    def project(i, carry):
        xs = []
        for e in range(2):
            place = e * z.pairs + i
            xs.append(
                jnp.concatenate(
                    [ot[pl.ds(c * span + place, z.rows, stride=z.head_stride), :] for c in range(z.chunks)], axis=1
                )
            )
        x = jnp.concatenate(xs, axis=0).astype(bf16)
        w = jnp.concatenate([vu[2 * i], vu[2 * i + 1]], axis=1)
        y = jnp.dot(x, w, preferred_element_type=f32)
        for e in range(2):
            yt[pl.ds(e * z.pairs + i, z.rows, stride=z.head_stride), :] = y[
                e * z.rows : (e + 1) * z.rows, e * z.value : (e + 1) * z.value
            ]
        return carry

    sums_pair = []
    for g in range(2):
        lax.fori_loop(g * group, (g + 1) * group, project, 0, unroll=8)

        def other_rows(k, carry):
            base = (k * CORES + 1 - core) * z.head_stride + g * group
            pieces = [yt[pl.ds(base + e * z.pairs, group), :] for e in range(2)]
            sendp[g, k] = jnp.concatenate(pieces, axis=0).astype(bf16)
            return carry

        lax.fori_loop(0, z.chips, other_rows, 0, unroll=4)
        sums_pair.append(pair_copy(2 + g, sendp.at[g], part.at[g]))
        sums_pair[g].start()

    stat_pair.wait_recv()
    whole = jnp.where(lane_s < LANES // 2, stat[...], stat[...] + statp[...])
    for b in range(z.seqs):
        statf[b] = whole[b : b + 1]
    for c in sums_pair:
        c.wait_recv()

    def own_rows(k, carry):
        halves = [part[g, k].astype(f32) for g in range(2)]
        theirs = jnp.concatenate([halves[g][e * group : (e + 1) * group] for e in range(2) for g in range(2)], axis=0)
        send[k] = (yt[pl.ds((k * CORES + core) * z.head_stride, z.heads), :] + theirs).astype(bf16)
        return carry

    lax.fori_loop(0, z.chips, own_rows, 0, unroll=4)

    def sums_copy(i, source):
        return pltpu.make_async_remote_copy(
            src_ref=send.at[peer_chip(i)], dst_ref=recv.at[source], send_sem=es_sem.at[i], recv_sem=er_sem.at[i],
            device_id={"ctx": peer_chip(i) * CORES + core}, device_id_type=MESH,
        )

    def stat_copy(i, source):
        return pltpu.make_async_remote_copy(
            src_ref=statf.at[peer_chip(i)], dst_ref=statr.at[source], send_sem=ss_sem.at[i], recv_sem=sr_sem.at[i],
            device_id={"ctx": peer_chip(i) * CORES + core}, device_id_type=MESH,
        )

    for i in order:
        stat_copy(i, chip).start()
        sums_copy(i, chip).start()
    recv[chip] = send[chip]
    statr[chip] = statf[chip]

    for i in order:
        stat_copy(i, source_chip(i)).wait_recv()
        sums_copy(i, source_chip(i)).wait_recv()

    s = jnp.concatenate([statr[d] for d in range(z.chips)], axis=0)
    s = jnp.where(core == 0, s, pltpu.roll(s, LANES - z.heads, 1))
    t = pltpu.roll(s, LANES // 2, 1)
    top = jnp.max(s, axis=0, keepdims=True)
    factor = jnp.exp(s - top)
    total = jnp.sum(factor * t, axis=0, keepdims=True)
    lane_d = lax.broadcasted_iota(jnp.int32, (z.chips, LANES), 1)
    share = jnp.where(lane_d < z.heads, factor / jnp.where(lane_d < z.heads, total, 1.0), 0.0)
    share = jnp.transpose(jnp.concatenate([share, jnp.zeros((LANES - z.chips, LANES), f32)], axis=0))
    merged = jnp.zeros((z.heads, z.value), f32)
    for d in range(z.chips):
        merged = merged + share[0 : z.heads, d : d + 1] * recv[d].astype(f32)
    acc[...] = merged
    for h in range(z.heads):
        at = (h % 2) * z.pairs + h // 2
        out_ref[:, h * z.value : (h + 1) * z.value] = acc[at : at + 1, :].astype(out_ref.dtype)

    for i in order:
        on_layer(i % side, lower, lambda: gather_copy(i, own_slot).wait_send())
    for i in [0] + level:
        forward_copy(i, core).wait_send()
    for dz in layers:
        on_layer(dz, higher, lambda: layer_copy(dz, chip_z).wait_send())
        from_layer(dz, lower, lambda: forward_layer(dz, core).wait_send())
        for i in order:
            if i % side == dz:
                from_layer(dz, higher, lambda: forward_copy(i, core).wait_send())
    for i in order:
        stat_copy(i, chip).wait_send()
        sums_copy(i, chip).wait_send()
    for c in (top_copy, stat_pair, *sums_pair):
        c.wait_send()


def per_device(
    query_nope, query_rope, cache_latent, cache_rope, key_up, value_up, lengths, block_owner, block_number,
):
    ctx = lax.axis_size("ctx")
    heads, nope, latent = key_up.shape
    slots, block, _ = cache_latent.shape
    z = Sizes(
        ctx, query_nope.shape[0] * ctx, heads, nope, query_rope.shape[1] // heads, latent, value_up.shape[2],
        slots, block, lengths.shape[0],
    )
    any_spec = pl.BlockSpec(memory_space=pl.ANY)
    V, S, D = pltpu.VMEM, pltpu.SMEM, pltpu.SemaphoreType.DMA
    span = z.rows * z.head_stride
    side = math.isqrt(z.chips)
    scratch = [
        V(query_nope.shape, bf16), V(query_rope.shape, bf16), V(cache_latent.shape, bf16), V(cache_rope.shape, bf16),
        V(key_up.shape, bf16), V(value_up.shape, bf16), S(lengths.shape, jnp.int32), S(block_owner.shape, jnp.int32),
        S(block_number.shape, jnp.int32), V((1, slots), jnp.int32), V((8, LANES), jnp.int32), S((8, LANES), jnp.int32),
        V((z.rows, z.block_rows, LANES), bf16),
        V((z.block_rows, LANES), f32),
        V((z.rows * z.gather_stride, LANES), f32),
        V((slots, z.key_stride, LANES), f32),
        V((slots, latent, block), bf16),
        V((z.chunks * span, LANES), f32),
        V((z.seqs, z.queries, latent), bf16),
        V((z.seqs, z.queries, LANES), f32),
        V((slots, z.queries, block), f32),
        V((slots, z.queries, block), f32),
        V((z.seqs, z.queries, block), f32),
        V((z.seqs, z.queries, block), f32),
        V((slots, z.queries, block), f32),
        V((slots, z.queries, latent), f32),
        V((z.chunks * span, LANES), f32),
        V((span, LANES), f32),
        V((2, z.chips, heads // 2, z.value), bf16),
        V((2, z.chips, heads // 2, z.value), bf16),
        V((z.chips, heads, z.value), bf16),
        V((z.chips, heads, z.value), bf16),
        V((z.seqs, LANES), f32),
        V((z.seqs, LANES), f32),
        V((z.seqs, 1, LANES), f32),
        V((z.chips, 1, LANES), f32),
        V((heads, z.value), f32),
        D((10,)), D, pltpu.SemaphoreType.REGULAR((side,)), D((z.chips,)), D((z.chips,)), D((z.chips,)), D((z.chips,)),
        D((side,)), D((side,)), D((side,)), D((side,)),
        D((4,)), D((4,)),
        D((z.chips,)), D((z.chips,)), D((z.chips,)), D((z.chips,)),
    ]
    return pl.pallas_call(
        functools.partial(kernel, z),
        out_shape=jax.ShapeDtypeStruct((1, heads * z.value), bf16),
        in_specs=[any_spec] * 10,
        out_specs=pl.BlockSpec(memory_space=pltpu.VMEM),
        scratch_shapes=scratch,
        compiler_params=pltpu.CompilerParams(
            collective_id=0, has_side_effects=True, vmem_limit_bytes=64 * 1024 * 1024 - 65536
        ),
    )(
        query_nope, query_rope, cache_latent, cache_rope, key_up, value_up, lengths, block_owner,
        block_owner.reshape(1, slots), block_number,
    )


def solution(mesh):
    return jax.shard_map(
        per_device,
        mesh=mesh,
        in_specs=(
            P("ctx", "head"), P("ctx", "head"), P("ctx", None, None), P("ctx", None), P("head", None, None),
            P("head", None, None), P(), P("ctx"), P("ctx"),
        ),
        out_specs=P("ctx", "head"),
        check_vma=False,
    )
```

```python
import functools
import math

import jax
import jax.numpy as jnp
from jax import lax
from jax.experimental import pallas as pl
from jax.experimental.pallas import tpu as pltpu
from jax.sharding import PartitionSpec as P

MESH = pl.DeviceIdType.MESH
score_scale = 192.0 ** (-0.5) * (1.0 + 0.1 * math.log(40.0)) ** 2
floor_value = -1e30
f32 = jnp.float32
bf16 = jnp.bfloat16
LANES = 128
CORES = 2


def pad8(n):
    return (n + 7) // 8 * 8


class Sizes:
    def __init__(self, ctx, rows, heads, nope, rope, latent, value, slots, block, seqs):
        self.ctx, self.rows, self.heads = ctx, rows, heads
        self.nope, self.rope, self.latent, self.value = nope, rope, latent, value
        self.slots, self.block, self.seqs = slots, block, seqs
        self.chips = ctx // CORES
        self.tokens = rows // seqs
        self.pairs = heads // 2
        self.queries = self.tokens * heads
        self.chunks = latent // LANES
        self.block_rows = heads + self.pairs
        self.gather_stride = pad8(self.block_rows) + 4
        self.head_stride = heads + 4
        self.key_stride = block + 8


def kernel(
    z,
    qn_hbm, qr_hbm, lat_hbm, kr_hbm, ku_hbm, vu_hbm, len_hbm, own_hbm, ownrow_hbm, num_hbm,
    out_ref,
    qn, qr, lat, kr, ku, vu, len_s, own_s, num_s, own_v, meta_v, meta_s,
    gath, qstage, gathf, rk, kt, qlt, ql, qro, sc, mpre, mtop, mpart, lpre, opre, ot, yt,
    sendp, part, send, recv, stat, statp, statf, statr, acc, row_out,
    out_sem, load_sem, meta_sem, gs_sem, gr_sem, fs_sem, fr_sem, ps_sem, pr_sem, es_sem, er_sem, ss_sem, sr_sem,
):
    me = lax.axis_index("ctx")
    chip = me // CORES
    core = me - chip * CORES
    partner = chip * CORES + (1 - core)

    side = math.isqrt(z.chips)
    chip_x = chip // side
    chip_z = chip - chip_x * side

    def peer_chip(i):
        return lax.rem(chip_x + i // side, side) * side + lax.rem(chip_z + i % side, side)

    def source_chip(i):
        return lax.rem(chip_x + side - i // side, side) * side + lax.rem(chip_z + side - i % side, side)

    def hops(i):
        return min(i // side, side - i // side) + min(i % side, side - i % side)

    far_first = sorted(range(z.chips), key=lambda i: -hops(i))

    piece = z.slots // 4
    lat_parts = [
        (lat_hbm.at[pl.ds(k * piece, piece)], lat.at[pl.ds(k * piece, piece)]) for k in range(4)
    ]
    loads = [
        pltpu.make_async_copy(s, d, load_sem.at[k])
        for k, (s, d) in enumerate(
            [(qn_hbm, qn), (qr_hbm, qr), (ownrow_hbm, own_v), (len_hbm, len_s), (own_hbm, own_s),
             (num_hbm, num_s), (kr_hbm, kr), *lat_parts, (ku_hbm, ku), (vu_hbm, vu)]
        )
    ]
    ld_qn, ld_qr, ld_ownv, ld_len, ld_own, ld_num, ld_kr, *ld_lat, ld_ku, ld_vu = loads
    for c in loads:
        c.start()

    barrier = pltpu.get_barrier_semaphore()
    for i in range(z.chips):
        target = peer_chip(i) * CORES + core if i else partner
        pl.semaphore_signal(barrier, inc=1, device_id={"ctx": target}, device_id_type=MESH)

    ld_qn.wait()
    ld_qr.wait()
    for h in range(z.heads):
        qstage[h : h + 1, :] = qn[:, h * LANES : (h + 1) * LANES].astype(f32)
    for h in range(z.pairs):
        qstage[z.heads + h : z.heads + h + 1, :] = qr[:, h * LANES : (h + 1) * LANES].astype(f32)
    gath[core * z.chips + chip] = qstage[...].astype(bf16)

    pl.semaphore_wait(barrier, z.chips)

    own_slot = core * z.chips + chip

    def gather_copy(i):
        return pltpu.make_async_remote_copy(
            src_ref=gath.at[own_slot], dst_ref=gath.at[own_slot], send_sem=gs_sem, recv_sem=gr_sem,
            device_id={"ctx": peer_chip(i) * CORES + core}, device_id_type=MESH,
        )

    def all_copies(src, dst, send_sem, recv_sem):
        some = pl.ds(0, z.chips - 1)
        return pltpu.make_async_remote_copy(
            src_ref=src.at[some], dst_ref=dst.at[some], send_sem=send_sem, recv_sem=recv_sem,
            device_id={"ctx": partner}, device_id_type=MESH,
        )

    all_rows = all_copies(gath, gath, gs_sem, gr_sem)
    half_rows = gath.at[pl.ds(core * z.chips, z.chips)]
    forward = pltpu.make_async_remote_copy(
        src_ref=half_rows, dst_ref=half_rows, send_sem=fs_sem, recv_sem=fr_sem,
        device_id={"ctx": partner}, device_id_type=MESH,
    )

    order = [i for i in far_first if i]
    for i in order:
        gather_copy(i).start()

    ld_ownv.wait()
    n = z.slots
    own_row = jnp.broadcast_to(own_v[...], (n, n))
    row_i = lax.broadcasted_iota(jnp.int32, (n, n), 0)
    col_i = lax.broadcasted_iota(jnp.int32, (n, n), 1)
    key_row = own_row * n + col_i
    key_col = jnp.sum(jnp.where(row_i == col_i, key_row, 0), axis=1, keepdims=True)
    rank_col = jnp.sum(jnp.where(key_row < key_col, 1, 0), axis=1, keepdims=True)
    perm = jnp.sum(jnp.where(rank_col == col_i, row_i, 0), axis=0, keepdims=True)
    ends = jnp.sum(jnp.where(key_col < (col_i + 1) * n, 1, 0), axis=0, keepdims=True)
    meta_v[0:1, 0:n] = perm
    meta_v[1:2, 0:n] = ends
    meta_copy = pltpu.make_async_copy(meta_v, meta_s, meta_sem)
    meta_copy.start()

    ld_kr.wait()

    rkf = rk.reshape(n * z.key_stride, LANES)

    def spread_keys(j, carry):
        part = kr[:, pl.ds(pl.multiple_of(j * LANES, LANES), LANES)].astype(f32)
        rkf[pl.ds(2 * j, n, stride=z.key_stride), :] = part
        rkf[pl.ds(2 * j + 1, n, stride=z.key_stride), :] = pltpu.roll(part, z.rope, 1)
        return carry

    lax.fori_loop(0, z.block * z.rope // LANES, spread_keys, 0, unroll=4)

    def turn_keys(p, carry):
        kt[p] = jnp.transpose(lat[p])
        return carry

    for k in range(3):
        ld_lat[k].wait()
        lax.fori_loop(k * piece, (k + 1) * piece, turn_keys, 0, unroll=2)

    all_rows.wait_recv()
    forward.start()

    ld_lat[3].wait()
    lax.fori_loop(3 * piece, 4 * piece, turn_keys, 0, unroll=2)

    forward.wait_recv()

    for row in range(z.rows):
        gathf[pl.ds(row * z.gather_stride, z.block_rows), :] = gath[row % CORES * z.chips + row // CORES].astype(f32)

    ld_ku.wait()
    span = z.rows * z.head_stride

    def absorb(i, carry):
        for e in range(2):
            h = 2 * i + e
            x = gathf[pl.ds(h, z.rows, stride=z.gather_stride), :].astype(bf16)
            y = jnp.dot(x, ku[h], preferred_element_type=f32)
            place = e * z.pairs + i
            for c in range(z.chunks):
                qlt[pl.ds(c * span + place, z.rows, stride=z.head_stride), :] = y[:, c * LANES : (c + 1) * LANES]
        return carry

    lax.fori_loop(0, z.pairs, absorb, 0, unroll=8)

    lane_p = lax.broadcasted_iota(jnp.int32, (z.pairs, LANES), 1)

    def queries(b, carry):
        for j in range(z.tokens):
            r = b * z.tokens + j
            for c in range(z.chunks):
                start = c * span + r * z.head_stride
                ql[b, j * z.heads : (j + 1) * z.heads, c * LANES : (c + 1) * LANES] = qlt[
                    pl.ds(start, z.heads), :
                ].astype(bf16)
            both = gathf[pl.ds(r * z.gather_stride + z.heads, z.pairs), :]
            qro[b, j * z.heads : j * z.heads + z.pairs, :] = jnp.where(lane_p < z.rope, both, 0.0)
            other = pltpu.roll(both, z.rope, 1)
            qro[b, j * z.heads + z.pairs : (j + 1) * z.heads, :] = jnp.where(lane_p < z.rope, other, 0.0)
        return carry

    lax.fori_loop(0, z.seqs, queries, 0, unroll=4)

    for c in (ld_len, ld_own, ld_num):
        c.wait()
    meta_copy.wait()
    token = lax.broadcasted_iota(jnp.int32, (z.queries, z.block), 0) // z.heads
    place = lax.broadcasted_iota(jnp.int32, (z.queries, z.block), 1) - token
    contract_last = (((1,), (1,)), ((), ()))

    def score(g, carry):
        top, before = carry
        js = [2 * g, 2 * g + 1]
        ps = [meta_s[0, j] for j in js]
        os = [own_s[p] for p in ps]
        bs = [jnp.maximum(o, 0) for o in os]
        lhs = jnp.concatenate([ql[b] for b in bs], axis=0)
        rhs = jnp.concatenate([kt[p] for p in ps], axis=1)
        full = jnp.dot(lhs, rhs, preferred_element_type=f32)
        lhs = jnp.concatenate([qro[b] for b in bs], axis=0)
        rhs = jnp.concatenate([rk[p, 0 : z.block, :] for p in ps], axis=0)
        full = full + lax.dot_general(lhs, rhs, contract_last, preferred_element_type=f32)
        for u in range(2):
            p, o, j = ps[u], os[u], js[u]
            limit = jnp.where(o >= 0, len_s[bs[u]] - (z.tokens - 1) - num_s[p] * z.block, -z.tokens)
            s = full[u * z.queries : (u + 1) * z.queries, u * z.block : (u + 1) * z.block]
            s = jnp.where(place < limit, s * score_scale, floor_value)
            sc[j] = s
            top = jnp.maximum(jnp.where(o == before, top, floor_value), s)
            mpre[j] = top
            before = o
        return top, before

    lax.fori_loop(
        0, n // 2, score, (jnp.full((z.queries, z.block), floor_value, f32), jnp.int32(-2)), unroll=8
    )

    lane_q = lax.broadcasted_iota(jnp.int32, (z.queries, LANES), 1)

    def segment(b):
        end = meta_s[1, b]
        return jnp.maximum(end - 1, 0), end

    def has_any(b):
        last, end = segment(b)
        return (end > 0) & (own_s[meta_s[0, last]] == b)

    def tops(b, carry):
        last, _ = segment(b)
        m = jnp.max(mpre[last], axis=1, keepdims=True)
        mtop[b] = jnp.broadcast_to(jnp.where(has_any(b), m, floor_value), (z.queries, z.block))
        return carry

    lax.fori_loop(0, z.seqs, tops, 0, unroll=4)

    def pair_copy(k, src, dst):
        return pltpu.make_async_remote_copy(
            src_ref=src, dst_ref=dst, send_sem=ps_sem.at[k], recv_sem=pr_sem.at[k],
            device_id={"ctx": partner}, device_id_type=MESH,
        )

    top_copy = pair_copy(0, mtop, mpart)
    top_copy.start()

    def weigh(j, carry):
        total, run, before = carry
        p = meta_s[0, j]
        o = own_s[p]
        b = jnp.maximum(o, 0)
        w = jnp.exp(sc[j] - mtop[b])
        keep = o == before
        total = jnp.where(keep, total, 0.0) + w
        lpre[j] = total
        run = jnp.where(keep, run, 0.0) + jnp.dot(w.astype(bf16), lat[p], preferred_element_type=f32)
        opre[j] = run
        return total, run, o

    lax.fori_loop(0, n, weigh, (jnp.zeros((z.queries, z.block), f32), jnp.zeros((z.queries, z.latent), f32), jnp.int32(-2)), unroll=16)

    top_copy.wait_recv()

    def finish(b, stats):
        last, _ = segment(b)
        mine = mtop[b]
        pair = jnp.maximum(mine, mpart[b])
        scale = jnp.exp(mine - pair)
        t = jnp.sum(lpre[last] * scale, axis=1, keepdims=True)
        for j in range(z.tokens):
            r = b * z.tokens + j
            for c in range(z.chunks):
                start = c * span + r * z.head_stride
                ot[pl.ds(start, z.heads), :] = (
                    opre[last, j * z.heads : (j + 1) * z.heads, c * LANES : (c + 1) * LANES]
                    * scale[j * z.heads : (j + 1) * z.heads]
                )
        stats = jnp.where(lane_q == b, pair, stats)
        return jnp.where(lane_q == z.seqs + b, t, stats)

    stats = lax.fori_loop(0, z.seqs, finish, jnp.zeros((z.queries, LANES), f32), unroll=4)
    turned = jnp.transpose(jnp.concatenate([stats, jnp.zeros((LANES - z.queries, LANES), f32)], axis=0))
    lane_s = lax.broadcasted_iota(jnp.int32, (z.seqs, LANES), 1)
    stat[...] = jnp.where(
        lane_s < LANES // 2, turned[0 : z.seqs], pltpu.roll(turned[z.seqs : 2 * z.seqs], LANES // 2, 1)
    )
    stat_pair = pair_copy(1, stat, statp)
    stat_pair.start()

    ld_vu.wait()
    group = z.pairs // 2

    def project(i, carry):
        xs = []
        for e in range(2):
            place = e * z.pairs + i
            xs.append(
                jnp.concatenate(
                    [ot[pl.ds(c * span + place, z.rows, stride=z.head_stride), :] for c in range(z.chunks)], axis=1
                )
            )
        x = jnp.concatenate(xs, axis=0).astype(bf16)
        w = jnp.concatenate([vu[2 * i], vu[2 * i + 1]], axis=1)
        y = jnp.dot(x, w, preferred_element_type=f32)
        for e in range(2):
            yt[pl.ds(e * z.pairs + i, z.rows, stride=z.head_stride), :] = y[
                e * z.rows : (e + 1) * z.rows, e * z.value : (e + 1) * z.value
            ]
        return carry

    sums_pair = []
    for g in range(2):
        lax.fori_loop(g * group, (g + 1) * group, project, 0, unroll=8)

        def other_rows(k, carry):
            base = (k * CORES + 1 - core) * z.head_stride + g * group
            pieces = [yt[pl.ds(base + e * z.pairs, group), :] for e in range(2)]
            sendp[g, k] = jnp.concatenate(pieces, axis=0).astype(bf16)
            return carry

        lax.fori_loop(0, z.chips, other_rows, 0, unroll=4)
        sums_pair.append(pair_copy(2 + g, sendp.at[g], part.at[g]))
        sums_pair[g].start()

    stat_pair.wait_recv()
    whole = jnp.where(lane_s < LANES // 2, stat[...], stat[...] + statp[...])
    for b in range(z.seqs):
        statf[b] = whole[b : b + 1]
    for c in sums_pair:
        c.wait_recv()

    def own_rows(k, carry):
        halves = [part[g, k].astype(f32) for g in range(2)]
        theirs = jnp.concatenate([halves[g][e * group : (e + 1) * group] for e in range(2) for g in range(2)], axis=0)
        send[k] = (yt[pl.ds((k * CORES + core) * z.head_stride, z.heads), :] + theirs).astype(bf16)
        return carry

    lax.fori_loop(0, z.chips, own_rows, 0, unroll=4)

    def sums_copy(i, source):
        return pltpu.make_async_remote_copy(
            src_ref=send.at[peer_chip(i)], dst_ref=recv.at[source], send_sem=es_sem, recv_sem=er_sem,
            device_id={"ctx": peer_chip(i) * CORES + core}, device_id_type=MESH,
        )

    def stat_copy(i, source):
        return pltpu.make_async_remote_copy(
            src_ref=statf.at[peer_chip(i)], dst_ref=statr.at[source], send_sem=ss_sem, recv_sem=sr_sem,
            device_id={"ctx": peer_chip(i) * CORES + core}, device_id_type=MESH,
        )

    for i in order:
        stat_copy(i, chip).start()
        sums_copy(i, chip).start()
    recv[chip] = send[chip]
    statr[chip] = statf[chip]

    all_stats = all_copies(statf, statr, ss_sem, sr_sem)
    all_sums = all_copies(send, recv, es_sem, er_sem)
    all_stats.wait_recv()
    all_sums.wait_recv()

    s = jnp.concatenate([statr[d] for d in range(z.chips)], axis=0)
    s = jnp.where(core == 0, s, pltpu.roll(s, LANES - z.heads, 1))
    t = pltpu.roll(s, LANES // 2, 1)
    top = jnp.max(s, axis=0, keepdims=True)
    factor = jnp.exp(s - top)
    total = jnp.sum(factor * t, axis=0, keepdims=True)
    lane_d = lax.broadcasted_iota(jnp.int32, (z.chips, LANES), 1)
    share = jnp.where(lane_d < z.heads, factor / jnp.where(lane_d < z.heads, total, 1.0), 0.0)
    share = jnp.transpose(jnp.concatenate([share, jnp.zeros((LANES - z.chips, LANES), f32)], axis=0))
    merged = jnp.zeros((z.heads, z.value), f32)
    for d in range(z.chips):
        merged = merged + share[0 : z.heads, d : d + 1] * recv[d].astype(f32)
    acc[...] = merged
    for h in range(z.heads):
        at = (h % 2) * z.pairs + h // 2
        row_out[:, h * z.value : (h + 1) * z.value] = acc[at : at + 1, :].astype(out_ref.dtype)
    out_copy = pltpu.make_async_copy(row_out, out_ref, out_sem)
    out_copy.start()

    all_rows.wait_send()
    forward.wait_send()
    all_stats.wait_send()
    all_sums.wait_send()
    for c in (top_copy, stat_pair, *sums_pair):
        c.wait_send()
    out_copy.wait()


def per_device(
    query_nope, query_rope, cache_latent, cache_rope, key_up, value_up, lengths, block_owner, block_number,
):
    ctx = lax.axis_size("ctx")
    heads, nope, latent = key_up.shape
    slots, block, _ = cache_latent.shape
    z = Sizes(
        ctx, query_nope.shape[0] * ctx, heads, nope, query_rope.shape[1] // heads, latent, value_up.shape[2],
        slots, block, lengths.shape[0],
    )
    any_spec = pl.BlockSpec(memory_space=pl.ANY)
    V, S, D = pltpu.VMEM, pltpu.SMEM, pltpu.SemaphoreType.DMA
    span = z.rows * z.head_stride
    scratch = [
        V(query_nope.shape, bf16), V(query_rope.shape, bf16), V(cache_latent.shape, bf16), V(cache_rope.shape, bf16),
        V(key_up.shape, bf16), V(value_up.shape, bf16), S(lengths.shape, jnp.int32), S(block_owner.shape, jnp.int32),
        S(block_number.shape, jnp.int32), V((1, slots), jnp.int32), V((8, LANES), jnp.int32), S((8, LANES), jnp.int32),
        V((z.rows, z.block_rows, LANES), bf16),
        V((z.block_rows, LANES), f32),
        V((z.rows * z.gather_stride, LANES), f32),
        V((slots, z.key_stride, LANES), f32),
        V((slots, latent, block), bf16),
        V((z.chunks * span, LANES), f32),
        V((z.seqs, z.queries, latent), bf16),
        V((z.seqs, z.queries, LANES), f32),
        V((slots, z.queries, block), f32),
        V((slots, z.queries, block), f32),
        V((z.seqs, z.queries, block), f32),
        V((z.seqs, z.queries, block), f32),
        V((slots, z.queries, block), f32),
        V((slots, z.queries, latent), f32),
        V((z.chunks * span, LANES), f32),
        V((span, LANES), f32),
        V((2, z.chips, heads // 2, z.value), bf16),
        V((2, z.chips, heads // 2, z.value), bf16),
        V((z.chips, heads, z.value), bf16),
        V((z.chips, heads, z.value), bf16),
        V((z.seqs, LANES), f32),
        V((z.seqs, LANES), f32),
        V((z.seqs, 1, LANES), f32),
        V((z.chips, 1, LANES), f32),
        V((heads, z.value), f32),
        V((1, heads * z.value), bf16),
        D,
        D((13,)), D, D, D, D, D,
        D((4,)), D((4,)),
        D, D, D, D,
    ]
    return pl.pallas_call(
        functools.partial(kernel, z),
        out_shape=jax.ShapeDtypeStruct((1, heads * z.value), bf16),
        in_specs=[any_spec] * 10,
        out_specs=any_spec,
        scratch_shapes=scratch,
        compiler_params=pltpu.CompilerParams(
            collective_id=0, has_side_effects=True, vmem_limit_bytes=64 * 1024 * 1024 - 65536
        ),
    )(
        query_nope, query_rope, cache_latent, cache_rope, key_up, value_up, lengths, block_owner,
        block_owner.reshape(1, slots), block_number,
    )


def solution(mesh):
    return jax.shard_map(
        per_device,
        mesh=mesh,
        in_specs=(
            P("ctx", "head"), P("ctx", "head"), P("ctx", None, None), P("ctx", None), P("head", None, None),
            P("head", None, None), P(), P("ctx"), P("ctx"),
        ),
        out_specs=P("ctx", "head"),
        check_vma=False,
    )
```

```python
import functools
import math

import jax
import jax.numpy as jnp
from jax import lax
from jax.experimental import pallas as pl
from jax.experimental.pallas import tpu as pltpu
from jax.sharding import PartitionSpec as P

MESH = pl.DeviceIdType.MESH
score_scale = 192.0 ** (-0.5) * (1.0 + 0.1 * math.log(40.0)) ** 2
floor_value = -1e30
f32 = jnp.float32
bf16 = jnp.bfloat16
LANES = 128
CORES = 2


def pad8(n):
    return (n + 7) // 8 * 8


class Sizes:
    def __init__(self, ctx, rows, heads, nope, rope, latent, value, slots, block, seqs):
        self.ctx, self.rows, self.heads = ctx, rows, heads
        self.nope, self.rope, self.latent, self.value = nope, rope, latent, value
        self.slots, self.block, self.seqs = slots, block, seqs
        self.chips = ctx // CORES
        self.tokens = rows // seqs
        self.pairs = heads // 2
        self.queries = self.tokens * heads
        self.chunks = latent // LANES
        self.block_rows = heads + self.pairs
        self.gather_stride = pad8(self.block_rows) + 4
        self.head_stride = heads + 4
        self.key_stride = block + 8


def kernel(
    z,
    qn_hbm, qr_hbm, lat_hbm, kr_hbm, ku_hbm, vu_hbm, len_hbm, own_hbm, ownrow_hbm, num_hbm,
    out_ref,
    qn, qr, lat, kr, ku, vu, len_s, own_s, num_s, own_v, meta_v, meta_s,
    gath, qstage, gathf, rk, kt, qlt, ql, qro, sc, mpre, mtop, mpart, lpre, opre, ot, yt,
    sendp, part, send, recv, stat, statp, statf, statr, shares, acc, row_out,
    out_sem, load_sem, meta_sem, gs_sem, gr_sem, fs_sem, fr_sem, ps_sem, pr_sem, es_sem, er_sem, ss_sem, sr_sem,
):
    me = lax.axis_index("ctx")
    chip = me // CORES
    core = me - chip * CORES
    partner = chip * CORES + (1 - core)

    side = math.isqrt(z.chips)
    chip_x = chip // side
    chip_z = chip - chip_x * side

    def peer_chip(i):
        return lax.rem(chip_x + i // side, side) * side + lax.rem(chip_z + i % side, side)

    def source_chip(i):
        return lax.rem(chip_x + side - i // side, side) * side + lax.rem(chip_z + side - i % side, side)

    def hops(i):
        return min(i // side, side - i // side) + min(i % side, side - i % side)

    far_first = sorted(range(z.chips), key=lambda i: -hops(i))

    piece = z.slots // 4
    lat_parts = [
        (lat_hbm.at[pl.ds(k * piece, piece)], lat.at[pl.ds(k * piece, piece)]) for k in range(4)
    ]
    loads = [
        pltpu.make_async_copy(s, d, load_sem.at[k])
        for k, (s, d) in enumerate(
            [(qn_hbm, qn), (qr_hbm, qr), (ownrow_hbm, own_v), (len_hbm, len_s), (own_hbm, own_s),
             (num_hbm, num_s), (kr_hbm, kr), *lat_parts, (ku_hbm, ku), (vu_hbm, vu)]
        )
    ]
    ld_qn, ld_qr, ld_ownv, ld_len, ld_own, ld_num, ld_kr, *ld_lat, ld_ku, ld_vu = loads
    for c in loads:
        c.start()

    barrier = pltpu.get_barrier_semaphore()
    for i in range(z.chips):
        target = peer_chip(i) * CORES + core if i else partner
        pl.semaphore_signal(barrier, inc=1, device_id={"ctx": target}, device_id_type=MESH)

    ld_qn.wait()
    ld_qr.wait()
    for h in range(z.heads):
        qstage[h : h + 1, :] = qn[:, h * LANES : (h + 1) * LANES].astype(f32)
    for h in range(z.pairs):
        qstage[z.heads + h : z.heads + h + 1, :] = qr[:, h * LANES : (h + 1) * LANES].astype(f32)
    gath[core * z.chips + chip] = qstage[...].astype(bf16)

    pl.semaphore_wait(barrier, z.chips)

    own_slot = core * z.chips + chip

    def gather_copy(i):
        return pltpu.make_async_remote_copy(
            src_ref=gath.at[own_slot], dst_ref=gath.at[own_slot], send_sem=gs_sem, recv_sem=gr_sem,
            device_id={"ctx": peer_chip(i) * CORES + core}, device_id_type=MESH,
        )

    def all_copies(src, dst, send_sem, recv_sem):
        some = pl.ds(0, z.chips - 1)
        return pltpu.make_async_remote_copy(
            src_ref=src.at[some], dst_ref=dst.at[some], send_sem=send_sem, recv_sem=recv_sem,
            device_id={"ctx": partner}, device_id_type=MESH,
        )

    all_rows = all_copies(gath, gath, gs_sem, gr_sem)
    half_rows = gath.at[pl.ds(core * z.chips, z.chips)]
    forward = pltpu.make_async_remote_copy(
        src_ref=half_rows, dst_ref=half_rows, send_sem=fs_sem, recv_sem=fr_sem,
        device_id={"ctx": partner}, device_id_type=MESH,
    )

    order = [i for i in far_first if i]
    late_first = sorted(range(z.chips), key=lambda k: (-(k % side), k // side in (0, 1)))
    for k in late_first:

        def give():
            pltpu.make_async_remote_copy(
                src_ref=gath.at[own_slot], dst_ref=gath.at[own_slot], send_sem=gs_sem, recv_sem=gr_sem,
                device_id={"ctx": k * CORES + core}, device_id_type=MESH,
            ).start()

        pl.when(chip != k)(give)

    ld_ownv.wait()
    n = z.slots
    own_row = jnp.broadcast_to(own_v[...], (n, n))
    row_i = lax.broadcasted_iota(jnp.int32, (n, n), 0)
    col_i = lax.broadcasted_iota(jnp.int32, (n, n), 1)
    key_row = own_row * n + col_i
    key_col = jnp.sum(jnp.where(row_i == col_i, key_row, 0), axis=1, keepdims=True)
    rank_col = jnp.sum(jnp.where(key_row < key_col, 1, 0), axis=1, keepdims=True)
    perm = jnp.sum(jnp.where(rank_col == col_i, row_i, 0), axis=0, keepdims=True)
    ends = jnp.sum(jnp.where(key_col < (col_i + 1) * n, 1, 0), axis=0, keepdims=True)
    meta_v[0:1, 0:n] = perm
    meta_v[1:2, 0:n] = ends
    meta_copy = pltpu.make_async_copy(meta_v, meta_s, meta_sem)
    meta_copy.start()

    ld_kr.wait()

    rkf = rk.reshape(n * z.key_stride, LANES)

    def spread_keys(j, carry):
        part = kr[:, pl.ds(pl.multiple_of(j * LANES, LANES), LANES)].astype(f32)
        rkf[pl.ds(2 * j, n, stride=z.key_stride), :] = part
        rkf[pl.ds(2 * j + 1, n, stride=z.key_stride), :] = pltpu.roll(part, z.rope, 1)
        return carry

    lax.fori_loop(0, z.block * z.rope // LANES, spread_keys, 0, unroll=4)

    def turn_keys(p, carry):
        kt[p] = jnp.transpose(lat[p])
        return carry

    for k in range(3):
        ld_lat[k].wait()
        lax.fori_loop(k * piece, (k + 1) * piece, turn_keys, 0, unroll=2)

    all_rows.wait_recv()
    forward.start()

    ld_lat[3].wait()
    lax.fori_loop(3 * piece, 4 * piece, turn_keys, 0, unroll=2)

    forward.wait_recv()

    for row in range(z.rows):
        gathf[pl.ds(row * z.gather_stride, z.block_rows), :] = gath[row % CORES * z.chips + row // CORES].astype(f32)

    ld_ku.wait()
    span = z.rows * z.head_stride

    def absorb(i, carry):
        for e in range(2):
            h = 2 * i + e
            x = gathf[pl.ds(h, z.rows, stride=z.gather_stride), :].astype(bf16)
            y = jnp.dot(x, ku[h], preferred_element_type=f32)
            place = e * z.pairs + i
            for c in range(z.chunks):
                qlt[pl.ds(c * span + place, z.rows, stride=z.head_stride), :] = y[:, c * LANES : (c + 1) * LANES]
        return carry

    lax.fori_loop(0, z.pairs, absorb, 0, unroll=8)

    lane_p = lax.broadcasted_iota(jnp.int32, (z.pairs, LANES), 1)

    def queries(b, carry):
        for j in range(z.tokens):
            r = b * z.tokens + j
            for c in range(z.chunks):
                start = c * span + r * z.head_stride
                ql[b, j * z.heads : (j + 1) * z.heads, c * LANES : (c + 1) * LANES] = qlt[
                    pl.ds(start, z.heads), :
                ].astype(bf16)
            both = gathf[pl.ds(r * z.gather_stride + z.heads, z.pairs), :]
            qro[b, j * z.heads : j * z.heads + z.pairs, :] = jnp.where(lane_p < z.rope, both, 0.0)
            other = pltpu.roll(both, z.rope, 1)
            qro[b, j * z.heads + z.pairs : (j + 1) * z.heads, :] = jnp.where(lane_p < z.rope, other, 0.0)
        return carry

    lax.fori_loop(0, z.seqs, queries, 0, unroll=16)

    for c in (ld_len, ld_own, ld_num):
        c.wait()
    meta_copy.wait()
    token = lax.broadcasted_iota(jnp.int32, (z.queries, z.block), 0) // z.heads
    place = lax.broadcasted_iota(jnp.int32, (z.queries, z.block), 1) - token
    contract_last = (((1,), (1,)), ((), ()))

    def score(g, carry):
        top, before = carry
        js = [2 * g, 2 * g + 1]
        ps = [meta_s[0, j] for j in js]
        os = [own_s[p] for p in ps]
        bs = [jnp.maximum(o, 0) for o in os]
        lhs = jnp.concatenate([ql[b] for b in bs], axis=0)
        rhs = jnp.concatenate([kt[p] for p in ps], axis=1)
        full = jnp.dot(lhs, rhs, preferred_element_type=f32)
        lhs = jnp.concatenate([qro[b] for b in bs], axis=0)
        rhs = jnp.concatenate([rk[p, 0 : z.block, :] for p in ps], axis=0)
        full = full + lax.dot_general(lhs, rhs, contract_last, preferred_element_type=f32)
        for u in range(2):
            p, o, j = ps[u], os[u], js[u]
            limit = jnp.where(o >= 0, len_s[bs[u]] - (z.tokens - 1) - num_s[p] * z.block, -z.tokens)
            s = full[u * z.queries : (u + 1) * z.queries, u * z.block : (u + 1) * z.block]
            s = jnp.where(place < limit, s * score_scale, floor_value)
            sc[j] = s
            top = jnp.maximum(jnp.where(o == before, top, floor_value), s)
            mpre[j] = top
            before = o
        return top, before

    lax.fori_loop(
        0, n // 2, score, (jnp.full((z.queries, z.block), floor_value, f32), jnp.int32(-2)), unroll=8
    )

    lane_q = lax.broadcasted_iota(jnp.int32, (z.queries, LANES), 1)

    def segment(b):
        end = meta_s[1, b]
        return jnp.maximum(end - 1, 0), end

    def has_any(b):
        last, end = segment(b)
        return (end > 0) & (own_s[meta_s[0, last]] == b)

    def tops(b, carry):
        last, _ = segment(b)
        m = jnp.max(mpre[last], axis=1, keepdims=True)
        mtop[b] = jnp.broadcast_to(jnp.where(has_any(b), m, floor_value), (z.queries, z.block))
        return carry

    lax.fori_loop(0, z.seqs, tops, 0, unroll=16)

    def pair_copy(k, src, dst):
        return pltpu.make_async_remote_copy(
            src_ref=src, dst_ref=dst, send_sem=ps_sem.at[k], recv_sem=pr_sem.at[k],
            device_id={"ctx": partner}, device_id_type=MESH,
        )

    top_copy = pair_copy(0, mtop, mpart)
    top_copy.start()

    def weigh(j, carry):
        total, run, before = carry
        p = meta_s[0, j]
        o = own_s[p]
        b = jnp.maximum(o, 0)
        w = jnp.exp(sc[j] - mtop[b])
        keep = o == before
        total = jnp.where(keep, total, 0.0) + w
        lpre[j] = total
        run = jnp.where(keep, run, 0.0) + jnp.dot(w.astype(bf16), lat[p], preferred_element_type=f32)
        opre[j] = run
        return total, run, o

    lax.fori_loop(0, n, weigh, (jnp.zeros((z.queries, z.block), f32), jnp.zeros((z.queries, z.latent), f32), jnp.int32(-2)), unroll=16)

    top_copy.wait_recv()

    def finish(b, stats):
        last, _ = segment(b)
        mine = mtop[b]
        pair = jnp.maximum(mine, mpart[b])
        scale = jnp.exp(mine - pair)
        t = jnp.sum(lpre[last] * scale, axis=1, keepdims=True)
        for j in range(z.tokens):
            r = b * z.tokens + j
            for c in range(z.chunks):
                start = c * span + r * z.head_stride
                ot[pl.ds(start, z.heads), :] = (
                    opre[last, j * z.heads : (j + 1) * z.heads, c * LANES : (c + 1) * LANES]
                    * scale[j * z.heads : (j + 1) * z.heads]
                )
        stats = jnp.where(lane_q == b, pair, stats)
        return jnp.where(lane_q == z.seqs + b, t, stats)

    stats = lax.fori_loop(0, z.seqs, finish, jnp.zeros((z.queries, LANES), f32), unroll=8)
    turned = jnp.transpose(jnp.concatenate([stats, jnp.zeros((LANES - z.queries, LANES), f32)], axis=0))
    lane_s = lax.broadcasted_iota(jnp.int32, (z.seqs, LANES), 1)
    stat[...] = jnp.where(
        lane_s < LANES // 2, turned[0 : z.seqs], pltpu.roll(turned[z.seqs : 2 * z.seqs], LANES // 2, 1)
    )
    stat_pair = pair_copy(1, stat, statp)
    stat_pair.start()

    ld_vu.wait()
    group = z.pairs // 2

    def project(i, carry):
        xs = []
        for e in range(2):
            place = e * z.pairs + i
            xs.append(
                jnp.concatenate(
                    [ot[pl.ds(c * span + place, z.rows, stride=z.head_stride), :] for c in range(z.chunks)], axis=1
                )
            )
        x = jnp.concatenate(xs, axis=0).astype(bf16)
        w = jnp.concatenate([vu[2 * i], vu[2 * i + 1]], axis=1)
        y = jnp.dot(x, w, preferred_element_type=f32)
        for e in range(2):
            yt[pl.ds(e * z.pairs + i, z.rows, stride=z.head_stride), :] = y[
                e * z.rows : (e + 1) * z.rows, e * z.value : (e + 1) * z.value
            ]
        return carry

    sums_pair = []
    for g in range(2):
        lax.fori_loop(g * group, (g + 1) * group, project, 0, unroll=8)

        def other_rows(k, carry):
            base = (k * CORES + 1 - core) * z.head_stride + g * group
            pieces = [yt[pl.ds(base + e * z.pairs, group), :] for e in range(2)]
            sendp[g, k] = jnp.concatenate(pieces, axis=0).astype(bf16)
            return carry

        lax.fori_loop(0, z.chips, other_rows, 0, unroll=4)
        sums_pair.append(pair_copy(2 + g, sendp.at[g], part.at[g]))
        sums_pair[g].start()

    def sums_copy(i, source):
        return pltpu.make_async_remote_copy(
            src_ref=send.at[peer_chip(i)], dst_ref=recv.at[source], send_sem=es_sem, recv_sem=er_sem,
            device_id={"ctx": peer_chip(i) * CORES + core}, device_id_type=MESH,
        )

    def stat_copy(i, source):
        return pltpu.make_async_remote_copy(
            src_ref=statf.at[peer_chip(i)], dst_ref=statr.at[source], send_sem=ss_sem, recv_sem=sr_sem,
            device_id={"ctx": peer_chip(i) * CORES + core}, device_id_type=MESH,
        )

    stat_pair.wait_recv()
    whole = jnp.where(lane_s < LANES // 2, stat[...], stat[...] + statp[...])
    for b in range(z.seqs):
        statf[b] = whole[b : b + 1]
    for i in order:
        stat_copy(i, chip).start()
    statr[chip] = statf[chip]
    for c in sums_pair:
        c.wait_recv()

    def own_rows(k, carry):
        halves = [part[g, k].astype(f32) for g in range(2)]
        theirs = jnp.concatenate([halves[g][e * group : (e + 1) * group] for e in range(2) for g in range(2)], axis=0)
        send[k] = (yt[pl.ds((k * CORES + core) * z.head_stride, z.heads), :] + theirs).astype(bf16)
        return carry

    lax.fori_loop(0, z.chips, own_rows, 0, unroll=4)

    for i in order:
        sums_copy(i, chip).start()
    recv[chip] = send[chip]

    all_stats = all_copies(statf, statr, ss_sem, sr_sem)
    all_sums = all_copies(send, recv, es_sem, er_sem)
    all_stats.wait_recv()

    s = jnp.concatenate([statr[d] for d in range(z.chips)], axis=0)
    s = jnp.where(core == 0, s, pltpu.roll(s, LANES - z.heads, 1))
    t = pltpu.roll(s, LANES // 2, 1)
    top = jnp.max(s, axis=0, keepdims=True)
    factor = jnp.exp(s - top)
    total = jnp.sum(factor * t, axis=0, keepdims=True)
    lane_d = lax.broadcasted_iota(jnp.int32, (z.chips, LANES), 1)
    share = jnp.where(lane_d < z.heads, factor / jnp.where(lane_d < z.heads, total, 1.0), 0.0)
    share = jnp.transpose(jnp.concatenate([share, jnp.zeros((LANES - z.chips, LANES), f32)], axis=0))
    shares[...] = share
    all_sums.wait_recv()
    merged = jnp.zeros((z.heads, z.value), f32)
    for d in range(z.chips):
        merged = merged + shares[0 : z.heads, d : d + 1] * recv[d].astype(f32)
    acc[...] = merged
    for h in range(z.heads):
        at = (h % 2) * z.pairs + h // 2
        row_out[:, h * z.value : (h + 1) * z.value] = acc[at : at + 1, :].astype(out_ref.dtype)
    out_copy = pltpu.make_async_copy(row_out, out_ref, out_sem)
    out_copy.start()

    all_rows.wait_send()
    forward.wait_send()
    all_stats.wait_send()
    all_sums.wait_send()
    for c in (top_copy, stat_pair, *sums_pair):
        c.wait_send()
    out_copy.wait()


def per_device(
    query_nope, query_rope, cache_latent, cache_rope, key_up, value_up, lengths, block_owner, block_number,
):
    ctx = lax.axis_size("ctx")
    heads, nope, latent = key_up.shape
    slots, block, _ = cache_latent.shape
    z = Sizes(
        ctx, query_nope.shape[0] * ctx, heads, nope, query_rope.shape[1] // heads, latent, value_up.shape[2],
        slots, block, lengths.shape[0],
    )
    any_spec = pl.BlockSpec(memory_space=pl.ANY)
    V, S, D = pltpu.VMEM, pltpu.SMEM, pltpu.SemaphoreType.DMA
    span = z.rows * z.head_stride
    scratch = [
        V(query_nope.shape, bf16), V(query_rope.shape, bf16), V(cache_latent.shape, bf16), V(cache_rope.shape, bf16),
        V(key_up.shape, bf16), V(value_up.shape, bf16), S(lengths.shape, jnp.int32), S(block_owner.shape, jnp.int32),
        S(block_number.shape, jnp.int32), V((1, slots), jnp.int32), V((8, LANES), jnp.int32), S((8, LANES), jnp.int32),
        V((z.rows, z.block_rows, LANES), bf16),
        V((z.block_rows, LANES), f32),
        V((z.rows * z.gather_stride, LANES), f32),
        V((slots, z.key_stride, LANES), f32),
        V((slots, latent, block), bf16),
        V((z.chunks * span, LANES), f32),
        V((z.seqs, z.queries, latent), bf16),
        V((z.seqs, z.queries, LANES), f32),
        V((slots, z.queries, block), f32),
        V((slots, z.queries, block), f32),
        V((z.seqs, z.queries, block), f32),
        V((z.seqs, z.queries, block), f32),
        V((slots, z.queries, block), f32),
        V((slots, z.queries, latent), f32),
        V((z.chunks * span, LANES), f32),
        V((span, LANES), f32),
        V((2, z.chips, heads // 2, z.value), bf16),
        V((2, z.chips, heads // 2, z.value), bf16),
        V((z.chips, heads, z.value), bf16),
        V((z.chips, heads, z.value), bf16),
        V((z.seqs, LANES), f32),
        V((z.seqs, LANES), f32),
        V((z.seqs, 1, LANES), f32),
        V((z.chips, 1, LANES), f32),
        V((LANES, LANES), f32),
        V((heads, z.value), f32),
        V((1, heads * z.value), bf16),
        D,
        D((13,)), D, D, D, D, D,
        D((4,)), D((4,)),
        D, D, D, D,
    ]
    return pl.pallas_call(
        functools.partial(kernel, z),
        out_shape=jax.ShapeDtypeStruct((1, heads * z.value), bf16),
        in_specs=[any_spec] * 10,
        out_specs=any_spec,
        scratch_shapes=scratch,
        compiler_params=pltpu.CompilerParams(
            collective_id=0, has_side_effects=True, vmem_limit_bytes=64 * 1024 * 1024 - 65536
        ),
    )(
        query_nope, query_rope, cache_latent, cache_rope, key_up, value_up, lengths, block_owner,
        block_owner.reshape(1, slots), block_number,
    )


def solution(mesh):
    return jax.shard_map(
        per_device,
        mesh=mesh,
        in_specs=(
            P("ctx", "head"), P("ctx", "head"), P("ctx", None, None), P("ctx", None), P("head", None, None),
            P("head", None, None), P(), P("ctx"), P("ctx"),
        ),
        out_specs=P("ctx", "head"),
        check_vma=False,
    )
```

```python
import functools
import math

import jax
import jax.numpy as jnp
from jax import lax
from jax.experimental import pallas as pl
from jax.experimental.pallas import tpu as pltpu
from jax.sharding import PartitionSpec as P

MESH = pl.DeviceIdType.MESH
score_scale = 192.0 ** (-0.5) * (1.0 + 0.1 * math.log(40.0)) ** 2
floor_value = -1e30
f32 = jnp.float32
bf16 = jnp.bfloat16
LANES = 128
CORES = 2


def pad8(n):
    return (n + 7) // 8 * 8


class Sizes:
    def __init__(self, ctx, rows, heads, nope, rope, latent, value, slots, block, seqs):
        self.ctx, self.rows, self.heads = ctx, rows, heads
        self.nope, self.rope, self.latent, self.value = nope, rope, latent, value
        self.slots, self.block, self.seqs = slots, block, seqs
        self.chips = ctx // CORES
        self.tokens = rows // seqs
        self.pairs = heads // 2
        self.queries = self.tokens * heads
        self.chunks = latent // LANES
        self.block_rows = heads + self.pairs
        self.gather_stride = pad8(self.block_rows) + 4
        self.head_stride = heads + 4
        self.key_stride = block + 8


def kernel(
    z,
    qn_hbm, qr_hbm, lat_hbm, kr_hbm, ku_hbm, vu_hbm, len_hbm, own_hbm, ownrow_hbm, num_hbm,
    out_ref,
    qn, qr, lat, kr, ku, vu, len_s, own_s, num_s, own_v, meta_v, meta_s,
    gath, qstage, gathf, rk, kt, qlt, ql, qro, sc, mpre, mtop, mtwo, mpart, lpre, opre, ot, yt,
    sendp, part, send, recv, stat, statp, statf, statr, shares, acc, row_out,
    out_sem, load_sem, meta_sem, gs_sem, gr_sem, fs_sem, fr_sem, ps_sem, pr_sem, es_sem, er_sem, ss_sem, sr_sem,
):
    me = lax.axis_index("ctx")
    chip = me // CORES
    core = me - chip * CORES
    partner = chip * CORES + (1 - core)

    side = math.isqrt(z.chips)
    chip_x = chip // side
    chip_z = chip - chip_x * side

    def peer_chip(i):
        return lax.rem(chip_x + i // side, side) * side + lax.rem(chip_z + i % side, side)

    def source_chip(i):
        return lax.rem(chip_x + side - i // side, side) * side + lax.rem(chip_z + side - i % side, side)

    def hops(i):
        return min(i // side, side - i // side) + min(i % side, side - i % side)

    far_first = sorted(range(z.chips), key=lambda i: -hops(i))

    piece = z.slots // 4
    lat_parts = [
        (lat_hbm.at[pl.ds(k * piece, piece)], lat.at[pl.ds(k * piece, piece)]) for k in range(4)
    ]
    loads = [
        pltpu.make_async_copy(s, d, load_sem.at[k])
        for k, (s, d) in enumerate(
            [(qn_hbm, qn), (qr_hbm, qr), (ownrow_hbm, own_v), (len_hbm, len_s), (own_hbm, own_s),
             (num_hbm, num_s), (kr_hbm, kr), *lat_parts, (ku_hbm, ku), (vu_hbm, vu)]
        )
    ]
    ld_qn, ld_qr, ld_ownv, ld_len, ld_own, ld_num, ld_kr, *ld_lat, ld_ku, ld_vu = loads
    for c in loads:
        c.start()

    barrier = pltpu.get_barrier_semaphore()
    for i in range(z.chips):
        target = peer_chip(i) * CORES + core if i else partner
        pl.semaphore_signal(barrier, inc=1, device_id={"ctx": target}, device_id_type=MESH)

    ld_qn.wait()
    ld_qr.wait()
    for h in range(z.heads):
        qstage[h : h + 1, :] = qn[:, h * LANES : (h + 1) * LANES].astype(f32)
    for h in range(z.pairs):
        qstage[z.heads + h : z.heads + h + 1, :] = qr[:, h * LANES : (h + 1) * LANES].astype(f32)
    gath[core * z.chips + chip] = qstage[...].astype(bf16)

    pl.semaphore_wait(barrier, z.chips)

    own_slot = core * z.chips + chip

    def gather_copy(i):
        return pltpu.make_async_remote_copy(
            src_ref=gath.at[own_slot], dst_ref=gath.at[own_slot], send_sem=gs_sem, recv_sem=gr_sem,
            device_id={"ctx": peer_chip(i) * CORES + core}, device_id_type=MESH,
        )

    def all_copies(src, dst, send_sem, recv_sem):
        some = pl.ds(0, z.chips - 1)
        return pltpu.make_async_remote_copy(
            src_ref=src.at[some], dst_ref=dst.at[some], send_sem=send_sem, recv_sem=recv_sem,
            device_id={"ctx": partner}, device_id_type=MESH,
        )

    all_rows = all_copies(gath, gath, gs_sem, gr_sem)
    half_rows = gath.at[pl.ds(core * z.chips, z.chips)]
    forward = pltpu.make_async_remote_copy(
        src_ref=half_rows, dst_ref=half_rows, send_sem=fs_sem, recv_sem=fr_sem,
        device_id={"ctx": partner}, device_id_type=MESH,
    )

    order = [i for i in far_first if i]
    def give(target):
        pltpu.make_async_remote_copy(
            src_ref=gath.at[own_slot], dst_ref=gath.at[own_slot], send_sem=gs_sem, recv_sem=gr_sem,
            device_id={"ctx": target * CORES + core}, device_id_type=MESH,
        ).start()

    def early():
        for k in sorted(range(z.chips), key=lambda k: (-(k % side), k // side in (0, 1))):
            pl.when(chip != k)(functools.partial(give, k))

    def late():
        for i in order:
            give(peer_chip(i))

    is_late = chip_z >= side // 2
    pl.when(is_late)(late)
    pl.when(jnp.logical_not(is_late))(early)

    ld_ownv.wait()
    n = z.slots
    own_row = jnp.broadcast_to(own_v[...], (n, n))
    row_i = lax.broadcasted_iota(jnp.int32, (n, n), 0)
    col_i = lax.broadcasted_iota(jnp.int32, (n, n), 1)
    key_row = own_row * n + col_i
    key_col = jnp.sum(jnp.where(row_i == col_i, key_row, 0), axis=1, keepdims=True)
    rank_col = jnp.sum(jnp.where(key_row < key_col, 1, 0), axis=1, keepdims=True)
    perm = jnp.sum(jnp.where(rank_col == col_i, row_i, 0), axis=0, keepdims=True)
    ends = jnp.sum(jnp.where(key_col < (col_i + 1) * n, 1, 0), axis=0, keepdims=True)
    meta_v[0:1, 0:n] = perm
    meta_v[1:2, 0:n] = ends
    meta_copy = pltpu.make_async_copy(meta_v, meta_s, meta_sem)
    meta_copy.start()

    ld_kr.wait()

    rkf = rk.reshape(n * z.key_stride, LANES)

    def spread_keys(j, carry):
        part = kr[:, pl.ds(pl.multiple_of(j * LANES, LANES), LANES)].astype(f32)
        rkf[pl.ds(2 * j, n, stride=z.key_stride), :] = part
        rkf[pl.ds(2 * j + 1, n, stride=z.key_stride), :] = pltpu.roll(part, z.rope, 1)
        return carry

    lax.fori_loop(0, z.block * z.rope // LANES, spread_keys, 0, unroll=4)

    def turn_keys(p, carry):
        kt[p] = jnp.transpose(lat[p])
        return carry

    for k in range(3):
        ld_lat[k].wait()
        lax.fori_loop(k * piece, (k + 1) * piece, turn_keys, 0, unroll=2)

    all_rows.wait_recv()
    forward.start()

    ld_lat[3].wait()
    lax.fori_loop(3 * piece, 4 * piece, turn_keys, 0, unroll=2)

    forward.wait_recv()

    for row in range(z.rows):
        gathf[pl.ds(row * z.gather_stride, z.block_rows), :] = gath[row % CORES * z.chips + row // CORES].astype(f32)

    ld_ku.wait()
    span = z.rows * z.head_stride

    def absorb(i, carry):
        for e in range(2):
            h = 2 * i + e
            x = gathf[pl.ds(h, z.rows, stride=z.gather_stride), :].astype(bf16)
            y = jnp.dot(x, ku[h], preferred_element_type=f32)
            place = e * z.pairs + i
            for c in range(z.chunks):
                qlt[pl.ds(c * span + place, z.rows, stride=z.head_stride), :] = y[:, c * LANES : (c + 1) * LANES]
        return carry

    lax.fori_loop(0, z.pairs, absorb, 0, unroll=16)

    lane_p = lax.broadcasted_iota(jnp.int32, (z.pairs, LANES), 1)

    def queries(b, carry):
        for j in range(z.tokens):
            r = b * z.tokens + j
            for c in range(z.chunks):
                start = c * span + r * z.head_stride
                ql[b, j * z.heads : (j + 1) * z.heads, c * LANES : (c + 1) * LANES] = qlt[
                    pl.ds(start, z.heads), :
                ].astype(bf16)
            both = gathf[pl.ds(r * z.gather_stride + z.heads, z.pairs), :]
            qro[b, j * z.heads : j * z.heads + z.pairs, :] = jnp.where(lane_p < z.rope, both, 0.0).astype(bf16)
            other = pltpu.roll(both, z.rope, 1)
            qro[b, j * z.heads + z.pairs : (j + 1) * z.heads, :] = jnp.where(lane_p < z.rope, other, 0.0).astype(bf16)
        return carry

    lax.fori_loop(0, z.seqs, queries, 0, unroll=16)

    for c in (ld_len, ld_own, ld_num):
        c.wait()
    meta_copy.wait()
    token = lax.broadcasted_iota(jnp.int32, (z.queries, z.block), 0) // z.heads
    place = lax.broadcasted_iota(jnp.int32, (z.queries, z.block), 1) - token
    contract_last = (((1,), (1,)), ((), ()))

    def score(g, carry):
        top, before = carry
        js = [2 * g, 2 * g + 1]
        ps = [meta_s[0, j] for j in js]
        os = [own_s[p] for p in ps]
        bs = [jnp.maximum(o, 0) for o in os]
        lhs = jnp.concatenate([ql[b] for b in bs], axis=0)
        rhs = jnp.concatenate([kt[p] for p in ps], axis=1)
        full = jnp.dot(lhs, rhs, preferred_element_type=f32)
        lhs = jnp.concatenate([qro[b] for b in bs], axis=0)
        rhs = jnp.concatenate([rk[p, 0 : z.block, :] for p in ps], axis=0).astype(bf16)
        full = full + lax.dot_general(lhs, rhs, contract_last, preferred_element_type=f32)
        for u in range(2):
            p, o, j = ps[u], os[u], js[u]
            limit = jnp.where(o >= 0, len_s[bs[u]] - (z.tokens - 1) - num_s[p] * z.block, -z.tokens)
            s = full[u * z.queries : (u + 1) * z.queries, u * z.block : (u + 1) * z.block]
            s = jnp.where(place < limit, s * score_scale, floor_value)
            sc[j] = s
            top = jnp.maximum(jnp.where(o == before, top, floor_value), s)
            mpre[j] = top
            before = o
        return top, before

    lax.fori_loop(
        0, n // 2, score, (jnp.full((z.queries, z.block), floor_value, f32), jnp.int32(-2)), unroll=32
    )

    lane_q = lax.broadcasted_iota(jnp.int32, (z.queries, LANES), 1)

    def segment(b):
        end = meta_s[1, b]
        return jnp.maximum(end - 1, 0), end

    def has_any(b):
        last, end = segment(b)
        return (end > 0) & (own_s[meta_s[0, last]] == b)

    low_q = lane_q < LANES // 2

    def tops(g, carry):
        two = []
        for b in (2 * g, 2 * g + 1):
            last, _ = segment(b)
            m = jnp.max(mpre[last], axis=1, keepdims=True)
            m = jnp.broadcast_to(jnp.where(has_any(b), m, floor_value), (z.queries, z.block))
            mtop[b] = m
            two.append(m)
        mtwo[g] = jnp.where(low_q, two[0], two[1])
        return carry

    lax.fori_loop(0, z.seqs // 2, tops, 0, unroll=8)

    def pair_copy(k, src, dst):
        return pltpu.make_async_remote_copy(
            src_ref=src, dst_ref=dst, send_sem=ps_sem.at[k], recv_sem=pr_sem.at[k],
            device_id={"ctx": partner}, device_id_type=MESH,
        )

    top_copy = pair_copy(0, mtwo, mpart)
    top_copy.start()

    def weigh(j, carry):
        total, run, before = carry
        p = meta_s[0, j]
        o = own_s[p]
        b = jnp.maximum(o, 0)
        w = jnp.exp(sc[j] - mtop[b])
        keep = o == before
        total = jnp.where(keep, total, 0.0) + w
        lpre[j] = total
        run = jnp.where(keep, run, 0.0) + jnp.dot(w.astype(bf16), lat[p], preferred_element_type=f32)
        opre[j] = run
        return total, run, o

    lax.fori_loop(0, n, weigh, (jnp.zeros((z.queries, z.block), f32), jnp.zeros((z.queries, z.latent), f32), jnp.int32(-2)), unroll=64)

    top_copy.wait_recv()

    def finish(g, stats):
        two = mpart[g]
        swapped = pltpu.roll(two, LANES // 2, 1)
        for e in range(2):
            b = 2 * g + e
            last, _ = segment(b)
            mine = mtop[b]
            pair = jnp.maximum(mine, jnp.where(low_q, two, swapped) if e == 0 else jnp.where(low_q, swapped, two))
            scale = jnp.exp(mine - pair)
            t = jnp.sum(lpre[last] * scale, axis=1, keepdims=True)
            for j in range(z.tokens):
                r = b * z.tokens + j
                for c in range(z.chunks):
                    start = c * span + r * z.head_stride
                    ot[pl.ds(start, z.heads), :] = (
                        opre[last, j * z.heads : (j + 1) * z.heads, c * LANES : (c + 1) * LANES]
                        * scale[j * z.heads : (j + 1) * z.heads]
                    )
            stats = jnp.where(lane_q == b, pair, stats)
            stats = jnp.where(lane_q == z.seqs + b, t, stats)
        return stats

    stats = lax.fori_loop(0, z.seqs // 2, finish, jnp.zeros((z.queries, LANES), f32), unroll=4)
    turned = jnp.transpose(jnp.concatenate([stats, jnp.zeros((LANES - z.queries, LANES), f32)], axis=0))
    lane_s = lax.broadcasted_iota(jnp.int32, (z.seqs, LANES), 1)
    stat[...] = jnp.where(
        lane_s < LANES // 2, turned[0 : z.seqs], pltpu.roll(turned[z.seqs : 2 * z.seqs], LANES // 2, 1)
    )
    stat_pair = pair_copy(1, stat, statp)
    stat_pair.start()

    ld_vu.wait()
    group = z.pairs // 2

    def project(i, carry):
        xs = []
        for e in range(2):
            place = e * z.pairs + i
            xs.append(
                jnp.concatenate(
                    [ot[pl.ds(c * span + place, z.rows, stride=z.head_stride), :] for c in range(z.chunks)], axis=1
                )
            )
        x = jnp.concatenate(xs, axis=0).astype(bf16)
        w = jnp.concatenate([vu[2 * i], vu[2 * i + 1]], axis=1)
        y = jnp.dot(x, w, preferred_element_type=f32)
        for e in range(2):
            yt[pl.ds(e * z.pairs + i, z.rows, stride=z.head_stride), :] = y[
                e * z.rows : (e + 1) * z.rows, e * z.value : (e + 1) * z.value
            ]
        return carry

    sums_pair = []
    for g in range(2):
        lax.fori_loop(g * group, (g + 1) * group, project, 0, unroll=8)

        def other_rows(k, carry):
            base = (k * CORES + 1 - core) * z.head_stride + g * group
            pieces = [yt[pl.ds(base + e * z.pairs, group), :] for e in range(2)]
            sendp[g, k] = jnp.concatenate(pieces, axis=0).astype(bf16)
            return carry

        lax.fori_loop(0, z.chips, other_rows, 0, unroll=16)
        sums_pair.append(pair_copy(2 + g, sendp.at[g], part.at[g]))
        sums_pair[g].start()

    def sums_copy(i, source):
        return pltpu.make_async_remote_copy(
            src_ref=send.at[peer_chip(i)], dst_ref=recv.at[source], send_sem=es_sem, recv_sem=er_sem,
            device_id={"ctx": peer_chip(i) * CORES + core}, device_id_type=MESH,
        )

    def stat_copy(i, source):
        return pltpu.make_async_remote_copy(
            src_ref=statf.at[peer_chip(i)], dst_ref=statr.at[source], send_sem=ss_sem, recv_sem=sr_sem,
            device_id={"ctx": peer_chip(i) * CORES + core}, device_id_type=MESH,
        )

    stat_pair.wait_recv()
    whole = jnp.where(lane_s < LANES // 2, stat[...], stat[...] + statp[...])
    for b in range(z.seqs):
        statf[b] = whole[b : b + 1]
    for i in order:
        stat_copy(i, chip).start()
    statr[chip] = statf[chip]
    for c in sums_pair:
        c.wait_recv()

    def own_rows(k, carry):
        halves = [part[g, k].astype(f32) for g in range(2)]
        theirs = jnp.concatenate([halves[g][e * group : (e + 1) * group] for e in range(2) for g in range(2)], axis=0)
        send[k] = (yt[pl.ds((k * CORES + core) * z.head_stride, z.heads), :] + theirs).astype(bf16)
        return carry

    lax.fori_loop(0, z.chips, own_rows, 0, unroll=16)

    for i in order:
        sums_copy(i, chip).start()
    recv[chip] = send[chip]

    all_stats = all_copies(statf, statr, ss_sem, sr_sem)
    all_sums = all_copies(send, recv, es_sem, er_sem)
    all_stats.wait_recv()

    s = jnp.concatenate([statr[d] for d in range(z.chips)], axis=0)
    s = jnp.where(core == 0, s, pltpu.roll(s, LANES - z.heads, 1))
    t = pltpu.roll(s, LANES // 2, 1)
    top = jnp.max(s, axis=0, keepdims=True)
    factor = jnp.exp(s - top)
    total = jnp.sum(factor * t, axis=0, keepdims=True)
    lane_d = lax.broadcasted_iota(jnp.int32, (z.chips, LANES), 1)
    share = jnp.where(lane_d < z.heads, factor / jnp.where(lane_d < z.heads, total, 1.0), 0.0)
    share = jnp.transpose(jnp.concatenate([share, jnp.zeros((LANES - z.chips, LANES), f32)], axis=0))
    shares[...] = share
    all_sums.wait_recv()
    merged = jnp.zeros((z.heads, z.value), f32)
    for d in range(z.chips):
        merged = merged + shares[0 : z.heads, d : d + 1] * recv[d].astype(f32)
    acc[...] = merged
    for h in range(z.heads):
        at = (h % 2) * z.pairs + h // 2
        row_out[:, h * z.value : (h + 1) * z.value] = acc[at : at + 1, :].astype(out_ref.dtype)
    out_copy = pltpu.make_async_copy(row_out, out_ref, out_sem)
    out_copy.start()

    all_rows.wait_send()
    forward.wait_send()
    all_stats.wait_send()
    all_sums.wait_send()
    for c in (top_copy, stat_pair, *sums_pair):
        c.wait_send()
    out_copy.wait()


def per_device(
    query_nope, query_rope, cache_latent, cache_rope, key_up, value_up, lengths, block_owner, block_number,
):
    ctx = lax.axis_size("ctx")
    heads, nope, latent = key_up.shape
    slots, block, _ = cache_latent.shape
    z = Sizes(
        ctx, query_nope.shape[0] * ctx, heads, nope, query_rope.shape[1] // heads, latent, value_up.shape[2],
        slots, block, lengths.shape[0],
    )
    any_spec = pl.BlockSpec(memory_space=pl.ANY)
    V, S, D = pltpu.VMEM, pltpu.SMEM, pltpu.SemaphoreType.DMA
    span = z.rows * z.head_stride
    scratch = [
        V(query_nope.shape, bf16), V(query_rope.shape, bf16), V(cache_latent.shape, bf16), V(cache_rope.shape, bf16),
        V(key_up.shape, bf16), V(value_up.shape, bf16), S(lengths.shape, jnp.int32), S(block_owner.shape, jnp.int32),
        S(block_number.shape, jnp.int32), V((1, slots), jnp.int32), V((8, LANES), jnp.int32), S((8, LANES), jnp.int32),
        V((z.rows, z.block_rows, LANES), bf16),
        V((z.block_rows, LANES), f32),
        V((z.rows * z.gather_stride, LANES), f32),
        V((slots, z.key_stride, LANES), f32),
        V((slots, latent, block), bf16),
        V((z.chunks * span, LANES), f32),
        V((z.seqs, z.queries, latent), bf16),
        V((z.seqs, z.queries, LANES), bf16),
        V((slots, z.queries, block), f32),
        V((slots, z.queries, block), f32),
        V((z.seqs, z.queries, block), f32),
        V((z.seqs // 2, z.queries, block), f32),
        V((z.seqs // 2, z.queries, block), f32),
        V((slots, z.queries, block), f32),
        V((slots, z.queries, latent), f32),
        V((z.chunks * span, LANES), f32),
        V((span, LANES), f32),
        V((2, z.chips, heads // 2, z.value), bf16),
        V((2, z.chips, heads // 2, z.value), bf16),
        V((z.chips, heads, z.value), bf16),
        V((z.chips, heads, z.value), bf16),
        V((z.seqs, LANES), f32),
        V((z.seqs, LANES), f32),
        V((z.seqs, 1, LANES), f32),
        V((z.chips, 1, LANES), f32),
        V((LANES, LANES), f32),
        V((heads, z.value), f32),
        V((1, heads * z.value), bf16),
        D,
        D((13,)), D, D, D, D, D,
        D((4,)), D((4,)),
        D, D, D, D,
    ]
    return pl.pallas_call(
        functools.partial(kernel, z),
        out_shape=jax.ShapeDtypeStruct((1, heads * z.value), bf16),
        in_specs=[any_spec] * 10,
        out_specs=any_spec,
        scratch_shapes=scratch,
        compiler_params=pltpu.CompilerParams(
            collective_id=0, has_side_effects=True, vmem_limit_bytes=64 * 1024 * 1024 - 65536
        ),
    )(
        query_nope, query_rope, cache_latent, cache_rope, key_up, value_up, lengths, block_owner,
        block_owner.reshape(1, slots), block_number,
    )


def solution(mesh):
    return jax.shard_map(
        per_device,
        mesh=mesh,
        in_specs=(
            P("ctx", "head"), P("ctx", "head"), P("ctx", None, None), P("ctx", None), P("head", None, None),
            P("head", None, None), P(), P("ctx"), P("ctx"),
        ),
        out_specs=P("ctx", "head"),
        check_vma=False,
    )
```

```python
import functools
import math

import jax
import jax.numpy as jnp
from jax import lax
from jax.experimental import pallas as pl
from jax.experimental.pallas import tpu as pltpu
from jax.sharding import PartitionSpec as P

MESH = pl.DeviceIdType.MESH
score_scale = 192.0 ** (-0.5) * (1.0 + 0.1 * math.log(40.0)) ** 2
floor_value = -1e30
f32 = jnp.float32
bf16 = jnp.bfloat16
LANES = 128
CORES = 2


def pad8(n):
    return (n + 7) // 8 * 8


class Sizes:
    def __init__(self, ctx, rows, heads, nope, rope, latent, value, slots, block, seqs):
        self.ctx, self.rows, self.heads = ctx, rows, heads
        self.nope, self.rope, self.latent, self.value = nope, rope, latent, value
        self.slots, self.block, self.seqs = slots, block, seqs
        self.chips = ctx // CORES
        self.tokens = rows // seqs
        self.pairs = heads // 2
        self.queries = self.tokens * heads
        self.chunks = latent // LANES
        self.block_rows = heads + self.pairs
        self.gather_stride = pad8(self.block_rows) + 4
        self.head_stride = heads + 4
        self.key_stride = block + 8


def kernel(
    z,
    qn_hbm, qr_hbm, lat_hbm, kr_hbm, ku_hbm, vu_hbm, len_hbm, own_hbm, ownrow_hbm, num_hbm,
    out_ref,
    qn, qr, lat, kr, ku, vu, len_s, own_s, num_s, own_v, meta_v, meta_s,
    gath, qown, qstage, gathf, rk, kt, qlt, ql, qro, sc, mpre, mtop, mpart, lpre, opre, ot, yt,
    sendp, part, send, recv, stat, statp, statf, statr, shares, acc, row_out,
    out_sem, load_sem, meta_sem, gs_sem, gr_sem, fs_sem, fr_sem, ps_sem, pr_sem, es_sem, er_sem, ss_sem, sr_sem,
):
    me = lax.axis_index("ctx")
    chip = me // CORES
    core = me - chip * CORES
    partner = chip * CORES + (1 - core)

    side = math.isqrt(z.chips)
    chip_x = chip // side
    chip_z = chip - chip_x * side

    def peer_chip(i):
        return lax.rem(chip_x + i // side, side) * side + lax.rem(chip_z + i % side, side)

    def source_chip(i):
        return lax.rem(chip_x + side - i // side, side) * side + lax.rem(chip_z + side - i % side, side)

    def hops(i):
        return min(i // side, side - i // side) + min(i % side, side - i % side)

    far_first = sorted(range(z.chips), key=lambda i: -hops(i))

    piece = z.slots // 4
    lat_parts = [
        (lat_hbm.at[pl.ds(k * piece, piece)], lat.at[pl.ds(k * piece, piece)]) for k in range(4)
    ]
    loads = [
        pltpu.make_async_copy(s, d, load_sem.at[k])
        for k, (s, d) in enumerate(
            [(qn_hbm, qn), (qr_hbm, qr), (ownrow_hbm, own_v), (len_hbm, len_s), (own_hbm, own_s),
             (num_hbm, num_s), (kr_hbm, kr), *lat_parts, (ku_hbm, ku), (vu_hbm, vu)]
        )
    ]
    ld_qn, ld_qr, ld_ownv, ld_len, ld_own, ld_num, ld_kr, *ld_lat, ld_ku, ld_vu = loads
    for c in loads:
        c.start()

    barrier = pltpu.get_barrier_semaphore()
    hub = core == 1

    def greet(device):
        pl.semaphore_signal(barrier, inc=1, device_id={"ctx": device}, device_id_type=MESH)

    def greet_all():
        for k in range(z.chips):
            greet(k * CORES)
            pl.when(chip != k)(functools.partial(greet, k * CORES + 1))

    pl.when(hub)(greet_all)
    pl.when(jnp.logical_not(hub))(functools.partial(greet, partner))

    ld_qn.wait()
    ld_qr.wait()
    for h in range(z.heads):
        qstage[h : h + 1, :] = qn[:, h * LANES : (h + 1) * LANES].astype(f32)
    for h in range(z.pairs):
        qstage[z.heads + h : z.heads + h + 1, :] = qr[:, h * LANES : (h + 1) * LANES].astype(f32)
    own_slot = core * z.chips + chip
    qown[...] = qstage[...].astype(bf16)
    gath[own_slot] = qown[...]

    pl.semaphore_wait(barrier, z.chips)

    def give(target):
        pltpu.make_async_remote_copy(
            src_ref=qown, dst_ref=gath.at[own_slot], send_sem=gs_sem, recv_sem=gr_sem.at[core],
            device_id={"ctx": target * CORES + 1}, device_id_type=MESH,
        ).start()

    def all_copies(count, src, dst, send_sem, recv_sem):
        some = pl.ds(0, count)
        return pltpu.make_async_remote_copy(
            src_ref=src.at[some], dst_ref=dst.at[some], send_sem=send_sem, recv_sem=recv_sem,
            device_id={"ctx": partner}, device_id_type=MESH,
        )

    rows_hub = all_copies(z.chips - 1, gath, gath, gs_sem, gr_sem.at[1])
    rows_leaf = all_copies(z.chips, gath, gath, gs_sem, gr_sem.at[0])

    def forward(kind):
        half = gath.at[pl.ds(kind * z.chips, z.chips)]
        return pltpu.make_async_remote_copy(
            src_ref=half, dst_ref=half, send_sem=fs_sem.at[kind], recv_sem=fr_sem.at[kind],
            device_id={"ctx": partner}, device_id_type=MESH,
        )

    order = [i for i in far_first if i]

    def early():
        for k in sorted(range(z.chips), key=lambda k: (-(k % side), k // side in (0, 1))):
            pl.when((chip != k) | (core == 0))(functools.partial(give, k))

    def late():
        for i in order:
            give(peer_chip(i))
        pl.when(core == 0)(functools.partial(give, chip))

    is_late = chip_z >= side // 2
    pl.when(is_late)(late)
    pl.when(jnp.logical_not(is_late))(early)

    ld_ownv.wait()
    n = z.slots
    own_row = jnp.broadcast_to(own_v[...], (n, n))
    row_i = lax.broadcasted_iota(jnp.int32, (n, n), 0)
    col_i = lax.broadcasted_iota(jnp.int32, (n, n), 1)
    key_row = own_row * n + col_i
    key_col = jnp.sum(jnp.where(row_i == col_i, key_row, 0), axis=1, keepdims=True)
    rank_col = jnp.sum(jnp.where(key_row < key_col, 1, 0), axis=1, keepdims=True)
    perm = jnp.sum(jnp.where(rank_col == col_i, row_i, 0), axis=0, keepdims=True)
    ends = jnp.sum(jnp.where(key_col < (col_i + 1) * n, 1, 0), axis=0, keepdims=True)
    meta_v[0:1, 0:n] = perm
    meta_v[1:2, 0:n] = ends
    meta_copy = pltpu.make_async_copy(meta_v, meta_s, meta_sem)
    meta_copy.start()

    ld_kr.wait()

    rkf = rk.reshape(n * z.key_stride, LANES)

    def spread_keys(j, carry):
        part = kr[:, pl.ds(pl.multiple_of(j * LANES, LANES), LANES)].astype(f32)
        rkf[pl.ds(2 * j, n, stride=z.key_stride), :] = part
        rkf[pl.ds(2 * j + 1, n, stride=z.key_stride), :] = pltpu.roll(part, z.rope, 1)
        return carry

    lax.fori_loop(0, z.block * z.rope // LANES, spread_keys, 0, unroll=4)

    def turn_keys(p, carry):
        kt[p] = jnp.transpose(lat[p])
        return carry

    for k in range(4):
        ld_lat[k].wait()
        lax.fori_loop(k * piece, (k + 1) * piece, turn_keys, 0, unroll=4)

    def hand_on():
        rows_hub.wait_recv()
        forward(1).start()
        rows_leaf.wait_recv()
        forward(0).start()

    pl.when(hub)(hand_on)

    def take():
        forward(1).wait_recv()
        forward(0).wait_recv()

    pl.when(jnp.logical_not(hub))(take)

    for row in range(z.rows):
        gathf[pl.ds(row * z.gather_stride, z.block_rows), :] = gath[row % CORES * z.chips + row // CORES].astype(f32)

    ld_ku.wait()
    span = z.rows * z.head_stride

    def absorb(i, carry):
        for e in range(2):
            h = 2 * i + e
            x = gathf[pl.ds(h, z.rows, stride=z.gather_stride), :].astype(bf16)
            y = jnp.dot(x, ku[h], preferred_element_type=f32)
            place = e * z.pairs + i
            for c in range(z.chunks):
                qlt[pl.ds(c * span + place, z.rows, stride=z.head_stride), :] = y[:, c * LANES : (c + 1) * LANES]
        return carry

    lax.fori_loop(0, z.pairs, absorb, 0, unroll=16)

    lane_p = lax.broadcasted_iota(jnp.int32, (z.pairs, LANES), 1)

    def queries(b, carry):
        for j in range(z.tokens):
            r = b * z.tokens + j
            for c in range(z.chunks):
                start = c * span + r * z.head_stride
                ql[b, j * z.heads : (j + 1) * z.heads, c * LANES : (c + 1) * LANES] = qlt[
                    pl.ds(start, z.heads), :
                ].astype(bf16)
            both = gathf[pl.ds(r * z.gather_stride + z.heads, z.pairs), :]
            qro[b, j * z.heads : j * z.heads + z.pairs, :] = jnp.where(lane_p < z.rope, both, 0.0).astype(bf16)
            other = pltpu.roll(both, z.rope, 1)
            qro[b, j * z.heads + z.pairs : (j + 1) * z.heads, :] = jnp.where(lane_p < z.rope, other, 0.0).astype(bf16)
        return carry

    lax.fori_loop(0, z.seqs, queries, 0, unroll=16)

    for c in (ld_len, ld_own, ld_num):
        c.wait()
    meta_copy.wait()
    token = lax.broadcasted_iota(jnp.int32, (z.queries, z.block), 0) // z.heads
    place = lax.broadcasted_iota(jnp.int32, (z.queries, z.block), 1) - token
    contract_last = (((1,), (1,)), ((), ()))

    def score(g, carry):
        top, before = carry
        js = [2 * g, 2 * g + 1]
        ps = [meta_s[0, j] for j in js]
        os = [own_s[p] for p in ps]
        bs = [jnp.maximum(o, 0) for o in os]
        lhs = jnp.concatenate([ql[b] for b in bs], axis=0)
        rhs = jnp.concatenate([kt[p] for p in ps], axis=1)
        full = jnp.dot(lhs, rhs, preferred_element_type=f32)
        lhs = jnp.concatenate([qro[b] for b in bs], axis=0)
        rhs = jnp.concatenate([rk[p, 0 : z.block, :] for p in ps], axis=0).astype(bf16)
        full = full + lax.dot_general(lhs, rhs, contract_last, preferred_element_type=f32)
        for u in range(2):
            p, o, j = ps[u], os[u], js[u]
            limit = jnp.where(o >= 0, len_s[bs[u]] - (z.tokens - 1) - num_s[p] * z.block, -z.tokens)
            s = full[u * z.queries : (u + 1) * z.queries, u * z.block : (u + 1) * z.block]
            s = jnp.where(place < limit, s * score_scale, floor_value)
            sc[j] = s
            top = jnp.maximum(jnp.where(o == before, top, floor_value), s)
            mpre[j] = top
            before = o
        return top, before

    lax.fori_loop(
        0, n // 2, score, (jnp.full((z.queries, z.block), floor_value, f32), jnp.int32(-2)), unroll=32
    )

    lane_q = lax.broadcasted_iota(jnp.int32, (z.queries, LANES), 1)

    def segment(b):
        end = meta_s[1, b]
        return jnp.maximum(end - 1, 0), end

    def has_any(b):
        last, end = segment(b)
        return (end > 0) & (own_s[meta_s[0, last]] == b)

    def tops(b, carry):
        last, _ = segment(b)
        m = jnp.max(mpre[last], axis=1, keepdims=True)
        mtop[b] = jnp.broadcast_to(jnp.where(has_any(b), m, floor_value), (z.queries, z.block))
        return carry

    lax.fori_loop(0, z.seqs, tops, 0, unroll=16)

    def pair_copy(k, src, dst):
        return pltpu.make_async_remote_copy(
            src_ref=src, dst_ref=dst, send_sem=ps_sem.at[k], recv_sem=pr_sem.at[k],
            device_id={"ctx": partner}, device_id_type=MESH,
        )

    top_copy = pair_copy(0, mtop, mpart)
    top_copy.start()

    def weigh(j, carry):
        total, run, before = carry
        p = meta_s[0, j]
        o = own_s[p]
        b = jnp.maximum(o, 0)
        w = jnp.exp(sc[j] - mtop[b])
        keep = o == before
        total = jnp.where(keep, total, 0.0) + w
        lpre[j] = total
        run = jnp.where(keep, run, 0.0) + jnp.dot(w.astype(bf16), lat[p], preferred_element_type=f32)
        opre[j] = run
        return total, run, o

    lax.fori_loop(0, n, weigh, (jnp.zeros((z.queries, z.block), f32), jnp.zeros((z.queries, z.latent), f32), jnp.int32(-2)), unroll=64)

    top_copy.wait_recv()

    def finish(b, stats):
        last, _ = segment(b)
        mine = mtop[b]
        pair = jnp.maximum(mine, mpart[b])
        scale = jnp.exp(mine - pair)
        t = jnp.sum(lpre[last] * scale, axis=1, keepdims=True)
        for j in range(z.tokens):
            r = b * z.tokens + j
            for c in range(z.chunks):
                start = c * span + r * z.head_stride
                ot[pl.ds(start, z.heads), :] = (
                    opre[last, j * z.heads : (j + 1) * z.heads, c * LANES : (c + 1) * LANES]
                    * scale[j * z.heads : (j + 1) * z.heads]
                )
        stats = jnp.where(lane_q == b, pair, stats)
        return jnp.where(lane_q == z.seqs + b, t, stats)

    stats = lax.fori_loop(0, z.seqs, finish, jnp.zeros((z.queries, LANES), f32), unroll=8)
    turned = jnp.transpose(jnp.concatenate([stats, jnp.zeros((LANES - z.queries, LANES), f32)], axis=0))
    lane_s = lax.broadcasted_iota(jnp.int32, (z.seqs, LANES), 1)
    stat[...] = jnp.where(
        lane_s < LANES // 2, turned[0 : z.seqs], pltpu.roll(turned[z.seqs : 2 * z.seqs], LANES // 2, 1)
    )
    stat_pair = pair_copy(1, stat, statp)
    stat_pair.start()

    ld_vu.wait()
    group = z.pairs // 2

    def project(i, carry):
        xs = []
        for e in range(2):
            place = e * z.pairs + i
            xs.append(
                jnp.concatenate(
                    [ot[pl.ds(c * span + place, z.rows, stride=z.head_stride), :] for c in range(z.chunks)], axis=1
                )
            )
        x = jnp.concatenate(xs, axis=0).astype(bf16)
        w = jnp.concatenate([vu[2 * i], vu[2 * i + 1]], axis=1)
        y = jnp.dot(x, w, preferred_element_type=f32)
        for e in range(2):
            yt[pl.ds(e * z.pairs + i, z.rows, stride=z.head_stride), :] = y[
                e * z.rows : (e + 1) * z.rows, e * z.value : (e + 1) * z.value
            ]
        return carry

    sums_pair = []
    for g in range(2):
        lax.fori_loop(g * group, (g + 1) * group, project, 0, unroll=8)

        def other_rows(k, carry):
            base = (k * CORES + 1 - core) * z.head_stride + g * group
            pieces = [yt[pl.ds(base + e * z.pairs, group), :] for e in range(2)]
            sendp[g, k] = jnp.concatenate(pieces, axis=0).astype(bf16)
            return carry

        lax.fori_loop(0, z.chips, other_rows, 0, unroll=16)
        sums_pair.append(pair_copy(2 + g, sendp.at[g], part.at[g]))
        sums_pair[g].start()

    def sums_copy(i, source):
        return pltpu.make_async_remote_copy(
            src_ref=send.at[peer_chip(i)], dst_ref=recv.at[source], send_sem=es_sem, recv_sem=er_sem,
            device_id={"ctx": peer_chip(i) * CORES + core}, device_id_type=MESH,
        )

    def stat_copy(i, source):
        return pltpu.make_async_remote_copy(
            src_ref=statf.at[peer_chip(i)], dst_ref=statr.at[source], send_sem=ss_sem, recv_sem=sr_sem,
            device_id={"ctx": peer_chip(i) * CORES + core}, device_id_type=MESH,
        )

    stat_pair.wait_recv()
    whole = jnp.where(lane_s < LANES // 2, stat[...], stat[...] + statp[...])
    for b in range(z.seqs):
        statf[b] = whole[b : b + 1]
    for i in order:
        stat_copy(i, chip).start()
    statr[chip] = statf[chip]
    for c in sums_pair:
        c.wait_recv()

    def own_rows(k, carry):
        halves = [part[g, k].astype(f32) for g in range(2)]
        theirs = jnp.concatenate([halves[g][e * group : (e + 1) * group] for e in range(2) for g in range(2)], axis=0)
        send[k] = (yt[pl.ds((k * CORES + core) * z.head_stride, z.heads), :] + theirs).astype(bf16)
        return carry

    lax.fori_loop(0, z.chips, own_rows, 0, unroll=16)

    for i in order:
        sums_copy(i, chip).start()
    recv[chip] = send[chip]

    all_stats = all_copies(z.chips - 1, statf, statr, ss_sem, sr_sem)
    all_sums = all_copies(z.chips - 1, send, recv, es_sem, er_sem)
    all_stats.wait_recv()

    s = jnp.concatenate([statr[d] for d in range(z.chips)], axis=0)
    s = jnp.where(core == 0, s, pltpu.roll(s, LANES - z.heads, 1))
    t = pltpu.roll(s, LANES // 2, 1)
    top = jnp.max(s, axis=0, keepdims=True)
    factor = jnp.exp(s - top)
    total = jnp.sum(factor * t, axis=0, keepdims=True)
    lane_d = lax.broadcasted_iota(jnp.int32, (z.chips, LANES), 1)
    share = jnp.where(lane_d < z.heads, factor / jnp.where(lane_d < z.heads, total, 1.0), 0.0)
    share = jnp.transpose(jnp.concatenate([share, jnp.zeros((LANES - z.chips, LANES), f32)], axis=0))
    shares[...] = share
    all_sums.wait_recv()
    merged = jnp.zeros((z.heads, z.value), f32)
    for d in range(z.chips):
        merged = merged + shares[0 : z.heads, d : d + 1] * recv[d].astype(f32)
    acc[...] = merged
    for h in range(z.heads):
        at = (h % 2) * z.pairs + h // 2
        row_out[:, h * z.value : (h + 1) * z.value] = acc[at : at + 1, :].astype(out_ref.dtype)
    out_copy = pltpu.make_async_copy(row_out, out_ref, out_sem)
    out_copy.start()

    def sent_hub():
        rows_hub.wait_send()
        forward(0).wait_send()
        forward(1).wait_send()

    pl.when(hub)(sent_hub)
    pl.when(jnp.logical_not(hub))(lambda: rows_leaf.wait_send())
    all_stats.wait_send()
    all_sums.wait_send()
    for c in (top_copy, stat_pair, *sums_pair):
        c.wait_send()
    out_copy.wait()


def per_device(
    query_nope, query_rope, cache_latent, cache_rope, key_up, value_up, lengths, block_owner, block_number,
):
    ctx = lax.axis_size("ctx")
    heads, nope, latent = key_up.shape
    slots, block, _ = cache_latent.shape
    z = Sizes(
        ctx, query_nope.shape[0] * ctx, heads, nope, query_rope.shape[1] // heads, latent, value_up.shape[2],
        slots, block, lengths.shape[0],
    )
    any_spec = pl.BlockSpec(memory_space=pl.ANY)
    V, S, D = pltpu.VMEM, pltpu.SMEM, pltpu.SemaphoreType.DMA
    span = z.rows * z.head_stride
    scratch = [
        V(query_nope.shape, bf16), V(query_rope.shape, bf16), V(cache_latent.shape, bf16), V(cache_rope.shape, bf16),
        V(key_up.shape, bf16), V(value_up.shape, bf16), S(lengths.shape, jnp.int32), S(block_owner.shape, jnp.int32),
        S(block_number.shape, jnp.int32), V((1, slots), jnp.int32), V((8, LANES), jnp.int32), S((8, LANES), jnp.int32),
        V((z.rows, z.block_rows, LANES), bf16),
        V((z.block_rows, LANES), bf16),
        V((z.block_rows, LANES), f32),
        V((z.rows * z.gather_stride, LANES), f32),
        V((slots, z.key_stride, LANES), f32),
        V((slots, latent, block), bf16),
        V((z.chunks * span, LANES), f32),
        V((z.seqs, z.queries, latent), bf16),
        V((z.seqs, z.queries, LANES), bf16),
        V((slots, z.queries, block), f32),
        V((slots, z.queries, block), f32),
        V((z.seqs, z.queries, block), f32),
        V((z.seqs, z.queries, block), f32),
        V((slots, z.queries, block), f32),
        V((slots, z.queries, latent), f32),
        V((z.chunks * span, LANES), f32),
        V((span, LANES), f32),
        V((2, z.chips, heads // 2, z.value), bf16),
        V((2, z.chips, heads // 2, z.value), bf16),
        V((z.chips, heads, z.value), bf16),
        V((z.chips, heads, z.value), bf16),
        V((z.seqs, LANES), f32),
        V((z.seqs, LANES), f32),
        V((z.seqs, 1, LANES), f32),
        V((z.chips, 1, LANES), f32),
        V((LANES, LANES), f32),
        V((heads, z.value), f32),
        V((1, heads * z.value), bf16),
        D,
        D((13,)), D, D, D((2,)), D((2,)), D((2,)),
        D((4,)), D((4,)),
        D, D, D, D,
    ]
    return pl.pallas_call(
        functools.partial(kernel, z),
        out_shape=jax.ShapeDtypeStruct((1, heads * z.value), bf16),
        in_specs=[any_spec] * 10,
        out_specs=any_spec,
        scratch_shapes=scratch,
        compiler_params=pltpu.CompilerParams(
            collective_id=0, has_side_effects=True, vmem_limit_bytes=64 * 1024 * 1024 - 65536
        ),
    )(
        query_nope, query_rope, cache_latent, cache_rope, key_up, value_up, lengths, block_owner,
        block_owner.reshape(1, slots), block_number,
    )


def solution(mesh):
    return jax.shard_map(
        per_device,
        mesh=mesh,
        in_specs=(
            P("ctx", "head"), P("ctx", "head"), P("ctx", None, None), P("ctx", None), P("head", None, None),
            P("head", None, None), P(), P("ctx"), P("ctx"),
        ),
        out_specs=P("ctx", "head"),
        check_vma=False,
    )
```

```python
import functools
import math

import jax
import jax.numpy as jnp
from jax import lax
from jax.experimental import pallas as pl
from jax.experimental.pallas import tpu as pltpu
from jax.sharding import PartitionSpec as P

MESH = pl.DeviceIdType.MESH
score_scale = 192.0 ** (-0.5) * (1.0 + 0.1 * math.log(40.0)) ** 2
floor_value = -1e30
f32 = jnp.float32
bf16 = jnp.bfloat16
LANES = 128
CORES = 2


def pad8(n):
    return (n + 7) // 8 * 8


class Sizes:
    def __init__(self, ctx, rows, heads, nope, rope, latent, value, slots, block, seqs):
        self.ctx, self.rows, self.heads = ctx, rows, heads
        self.nope, self.rope, self.latent, self.value = nope, rope, latent, value
        self.slots, self.block, self.seqs = slots, block, seqs
        self.chips = ctx // CORES
        self.tokens = rows // seqs
        self.pairs = heads // 2
        self.queries = self.tokens * heads
        self.chunks = latent // LANES
        self.block_rows = heads + self.pairs
        self.gather_stride = pad8(self.block_rows) + 4
        self.head_stride = heads + 4
        self.key_stride = block + 8


def kernel(
    z,
    qn_hbm, qr_hbm, lat_hbm, kr_hbm, ku_hbm, vu_hbm, len_hbm, own_hbm, ownrow_hbm, num_hbm,
    out_ref,
    qn, qr, lat, kr, ku, vu, len_s, own_s, num_s, own_v, meta_v, meta_s,
    gath, qown, qstage, gathf, rk, kt, qlt, ql, qro, sc, mpre, mtop, mpart, lpre, opre, ot, yt,
    sendp, part, send, recv, stat, statp, statf, statr, shares, acc, row_out,
    out_sem, load_sem, meta_sem, gs_sem, gr_sem, fs_sem, fr_sem, ps_sem, pr_sem, es_sem, er_sem, ss_sem, sr_sem,
):
    me = lax.axis_index("ctx")
    chip = me // CORES
    core = me - chip * CORES
    partner = chip * CORES + (1 - core)

    side = math.isqrt(z.chips)
    chip_x = chip // side
    chip_z = chip - chip_x * side

    def peer_chip(i):
        return lax.rem(chip_x + i // side, side) * side + lax.rem(chip_z + i % side, side)

    def source_chip(i):
        return lax.rem(chip_x + side - i // side, side) * side + lax.rem(chip_z + side - i % side, side)

    def hops(i):
        return min(i // side, side - i // side) + min(i % side, side - i % side)

    far_first = sorted(range(z.chips), key=lambda i: -hops(i))

    piece = z.slots // 4
    lat_parts = [
        (lat_hbm.at[pl.ds(k * piece, piece)], lat.at[pl.ds(k * piece, piece)]) for k in range(4)
    ]
    loads = [
        pltpu.make_async_copy(s, d, load_sem.at[k])
        for k, (s, d) in enumerate(
            [(qn_hbm, qn), (qr_hbm, qr), (ownrow_hbm, own_v), (len_hbm, len_s), (own_hbm, own_s),
             (num_hbm, num_s), (kr_hbm, kr), *lat_parts, (ku_hbm, ku), (vu_hbm, vu)]
        )
    ]
    ld_qn, ld_qr, ld_ownv, ld_len, ld_own, ld_num, ld_kr, *ld_lat, ld_ku, ld_vu = loads

    barrier = pltpu.get_barrier_semaphore()
    hub = core == 1

    def greet(device):
        pl.semaphore_signal(barrier, inc=1, device_id={"ctx": device}, device_id_type=MESH)

    def greet_all():
        for k in range(z.chips):
            greet(k * CORES)
            pl.when(chip != k)(functools.partial(greet, k * CORES + 1))

    pl.when(hub)(greet_all)
    pl.when(jnp.logical_not(hub))(functools.partial(greet, partner))
    for c in loads:
        c.start()

    ld_qn.wait()
    ld_qr.wait()
    for h in range(z.heads):
        qstage[h : h + 1, :] = qn[:, h * LANES : (h + 1) * LANES].astype(f32)
    for h in range(z.pairs):
        qstage[z.heads + h : z.heads + h + 1, :] = qr[:, h * LANES : (h + 1) * LANES].astype(f32)
    own_slot = core * z.chips + chip
    qown[...] = qstage[...].astype(bf16)
    gath[own_slot] = qown[...]

    pl.semaphore_wait(barrier, z.chips)

    def give(target):
        pltpu.make_async_remote_copy(
            src_ref=qown, dst_ref=gath.at[own_slot], send_sem=gs_sem, recv_sem=gr_sem.at[core],
            device_id={"ctx": target * CORES + 1}, device_id_type=MESH,
        ).start()

    def all_copies(count, src, dst, send_sem, recv_sem):
        some = pl.ds(0, count)
        return pltpu.make_async_remote_copy(
            src_ref=src.at[some], dst_ref=dst.at[some], send_sem=send_sem, recv_sem=recv_sem,
            device_id={"ctx": partner}, device_id_type=MESH,
        )

    rows_hub = all_copies(z.chips - 1, gath, gath, gs_sem, gr_sem.at[1])
    rows_leaf = all_copies(z.chips, gath, gath, gs_sem, gr_sem.at[0])

    def forward(kind):
        half = gath.at[pl.ds(kind * z.chips, z.chips)]
        return pltpu.make_async_remote_copy(
            src_ref=half, dst_ref=half, send_sem=fs_sem.at[kind], recv_sem=fr_sem.at[kind],
            device_id={"ctx": partner}, device_id_type=MESH,
        )

    order = [i for i in far_first if i]

    def early():
        for k in sorted(range(z.chips), key=lambda k: (-(k % side), k // side in (0, 1))):
            pl.when((chip != k) | (core == 0))(functools.partial(give, k))

    def late():
        for i in order:
            give(peer_chip(i))
        pl.when(core == 0)(functools.partial(give, chip))

    is_late = chip_z >= side // 2
    pl.when(is_late)(late)
    pl.when(jnp.logical_not(is_late))(early)

    ld_ownv.wait()
    n = z.slots
    own_row = jnp.broadcast_to(own_v[...], (n, n))
    row_i = lax.broadcasted_iota(jnp.int32, (n, n), 0)
    col_i = lax.broadcasted_iota(jnp.int32, (n, n), 1)
    key_row = own_row * n + col_i
    key_col = jnp.sum(jnp.where(row_i == col_i, key_row, 0), axis=1, keepdims=True)
    rank_col = jnp.sum(jnp.where(key_row < key_col, 1, 0), axis=1, keepdims=True)
    perm = jnp.sum(jnp.where(rank_col == col_i, row_i, 0), axis=0, keepdims=True)
    ends = jnp.sum(jnp.where(key_col < (col_i + 1) * n, 1, 0), axis=0, keepdims=True)
    meta_v[0:1, 0:n] = perm
    meta_v[1:2, 0:n] = ends
    meta_copy = pltpu.make_async_copy(meta_v, meta_s, meta_sem)
    meta_copy.start()

    ld_kr.wait()

    rkf = rk.reshape(n * z.key_stride, LANES)

    def spread_keys(j, carry):
        part = kr[:, pl.ds(pl.multiple_of(j * LANES, LANES), LANES)].astype(f32)
        rkf[pl.ds(2 * j, n, stride=z.key_stride), :] = part
        rkf[pl.ds(2 * j + 1, n, stride=z.key_stride), :] = pltpu.roll(part, z.rope, 1)
        return carry

    lax.fori_loop(0, z.block * z.rope // LANES, spread_keys, 0, unroll=4)

    def turn_keys(p, carry):
        kt[p] = jnp.transpose(lat[p])
        return carry

    for k in range(4):
        ld_lat[k].wait()
        lax.fori_loop(k * piece, (k + 1) * piece, turn_keys, 0, unroll=4)

    def hand_on():
        rows_hub.wait_recv()
        forward(1).start()
        rows_leaf.wait_recv()
        forward(0).start()

    pl.when(hub)(hand_on)

    def take():
        forward(1).wait_recv()
        forward(0).wait_recv()

    pl.when(jnp.logical_not(hub))(take)

    for row in range(z.rows):
        gathf[pl.ds(row * z.gather_stride, z.block_rows), :] = gath[row % CORES * z.chips + row // CORES].astype(f32)

    ld_ku.wait()
    span = z.rows * z.head_stride

    def absorb(i, carry):
        for e in range(2):
            h = 2 * i + e
            x = gathf[pl.ds(h, z.rows, stride=z.gather_stride), :].astype(bf16)
            y = jnp.dot(x, ku[h], preferred_element_type=f32)
            place = e * z.pairs + i
            for c in range(z.chunks):
                qlt[pl.ds(c * span + place, z.rows, stride=z.head_stride), :] = y[:, c * LANES : (c + 1) * LANES]
        return carry

    lax.fori_loop(0, z.pairs, absorb, 0, unroll=16)

    lane_p = lax.broadcasted_iota(jnp.int32, (z.pairs, LANES), 1)

    def queries(b, carry):
        for j in range(z.tokens):
            r = b * z.tokens + j
            for c in range(z.chunks):
                start = c * span + r * z.head_stride
                ql[b, j * z.heads : (j + 1) * z.heads, c * LANES : (c + 1) * LANES] = qlt[
                    pl.ds(start, z.heads), :
                ].astype(bf16)
            both = gathf[pl.ds(r * z.gather_stride + z.heads, z.pairs), :]
            qro[b, j * z.heads : j * z.heads + z.pairs, :] = jnp.where(lane_p < z.rope, both, 0.0).astype(bf16)
            other = pltpu.roll(both, z.rope, 1)
            qro[b, j * z.heads + z.pairs : (j + 1) * z.heads, :] = jnp.where(lane_p < z.rope, other, 0.0).astype(bf16)
        return carry

    lax.fori_loop(0, z.seqs, queries, 0, unroll=16)

    for c in (ld_len, ld_own, ld_num):
        c.wait()
    meta_copy.wait()
    token = lax.broadcasted_iota(jnp.int32, (z.queries, z.block), 0) // z.heads
    place = lax.broadcasted_iota(jnp.int32, (z.queries, z.block), 1) - token
    contract_last = (((1,), (1,)), ((), ()))

    def score(g, carry):
        top, before = carry
        js = [2 * g, 2 * g + 1]
        ps = [meta_s[0, j] for j in js]
        os = [own_s[p] for p in ps]
        bs = [jnp.maximum(o, 0) for o in os]
        lhs = jnp.concatenate([ql[b] for b in bs], axis=0)
        rhs = jnp.concatenate([kt[p] for p in ps], axis=1)
        full = jnp.dot(lhs, rhs, preferred_element_type=f32)
        lhs = jnp.concatenate([qro[b] for b in bs], axis=0)
        rhs = jnp.concatenate([rk[p, 0 : z.block, :] for p in ps], axis=0).astype(bf16)
        full = full + lax.dot_general(lhs, rhs, contract_last, preferred_element_type=f32)
        for u in range(2):
            p, o, j = ps[u], os[u], js[u]
            limit = jnp.where(o >= 0, len_s[bs[u]] - (z.tokens - 1) - num_s[p] * z.block, -z.tokens)
            s = full[u * z.queries : (u + 1) * z.queries, u * z.block : (u + 1) * z.block]
            s = jnp.where(place < limit, s * score_scale, floor_value)
            sc[j] = s
            top = jnp.maximum(jnp.where(o == before, top, floor_value), s)
            mpre[j] = top
            before = o
        return top, before

    lax.fori_loop(
        0, n // 2, score, (jnp.full((z.queries, z.block), floor_value, f32), jnp.int32(-2)), unroll=32
    )

    lane_q = lax.broadcasted_iota(jnp.int32, (z.queries, LANES), 1)

    def segment(b):
        end = meta_s[1, b]
        return jnp.maximum(end - 1, 0), end

    def has_any(b):
        last, end = segment(b)
        return (end > 0) & (own_s[meta_s[0, last]] == b)

    def tops(b, carry):
        last, _ = segment(b)
        m = jnp.max(mpre[last], axis=1, keepdims=True)
        mtop[b] = jnp.broadcast_to(jnp.where(has_any(b), m, floor_value), (z.queries, z.block))
        return carry

    lax.fori_loop(0, z.seqs, tops, 0, unroll=16)

    def pair_copy(k, src, dst):
        return pltpu.make_async_remote_copy(
            src_ref=src, dst_ref=dst, send_sem=ps_sem.at[k], recv_sem=pr_sem.at[k],
            device_id={"ctx": partner}, device_id_type=MESH,
        )

    top_copy = pair_copy(0, mtop, mpart)
    top_copy.start()

    def weigh(j, carry):
        total, run, before = carry
        p = meta_s[0, j]
        o = own_s[p]
        b = jnp.maximum(o, 0)
        w = jnp.exp(sc[j] - mtop[b])
        keep = o == before
        total = jnp.where(keep, total, 0.0) + w
        lpre[j] = total
        run = jnp.where(keep, run, 0.0) + jnp.dot(w.astype(bf16), lat[p], preferred_element_type=f32)
        opre[j] = run
        return total, run, o

    lax.fori_loop(0, n, weigh, (jnp.zeros((z.queries, z.block), f32), jnp.zeros((z.queries, z.latent), f32), jnp.int32(-2)), unroll=64)

    top_copy.wait_recv()

    def finish(b, stats):
        last, _ = segment(b)
        mine = mtop[b]
        pair = jnp.maximum(mine, mpart[b])
        scale = jnp.exp(mine - pair)
        t = jnp.sum(lpre[last] * scale, axis=1, keepdims=True)
        for j in range(z.tokens):
            r = b * z.tokens + j
            for c in range(z.chunks):
                start = c * span + r * z.head_stride
                ot[pl.ds(start, z.heads), :] = (
                    opre[last, j * z.heads : (j + 1) * z.heads, c * LANES : (c + 1) * LANES]
                    * scale[j * z.heads : (j + 1) * z.heads]
                )
        stats = jnp.where(lane_q == b, pair, stats)
        return jnp.where(lane_q == z.seqs + b, t, stats)

    stats = lax.fori_loop(0, z.seqs, finish, jnp.zeros((z.queries, LANES), f32), unroll=8)
    turned = jnp.transpose(jnp.concatenate([stats, jnp.zeros((LANES - z.queries, LANES), f32)], axis=0))
    lane_s = lax.broadcasted_iota(jnp.int32, (z.seqs, LANES), 1)
    stat[...] = jnp.where(
        lane_s < LANES // 2, turned[0 : z.seqs], pltpu.roll(turned[z.seqs : 2 * z.seqs], LANES // 2, 1)
    )
    stat_pair = pair_copy(1, stat, statp)
    stat_pair.start()

    ld_vu.wait()
    group = z.pairs // 2

    def project(i, carry):
        xs = []
        for e in range(2):
            place = e * z.pairs + i
            xs.append(
                jnp.concatenate(
                    [ot[pl.ds(c * span + place, z.rows, stride=z.head_stride), :] for c in range(z.chunks)], axis=1
                )
            )
        x = jnp.concatenate(xs, axis=0).astype(bf16)
        w = jnp.concatenate([vu[2 * i], vu[2 * i + 1]], axis=1)
        y = jnp.dot(x, w, preferred_element_type=f32)
        for e in range(2):
            yt[pl.ds(e * z.pairs + i, z.rows, stride=z.head_stride), :] = y[
                e * z.rows : (e + 1) * z.rows, e * z.value : (e + 1) * z.value
            ]
        return carry

    sums_pair = []
    for g in range(2):
        lax.fori_loop(g * group, (g + 1) * group, project, 0, unroll=8)

        def other_rows(k, carry):
            base = (k * CORES + 1 - core) * z.head_stride + g * group
            pieces = [yt[pl.ds(base + e * z.pairs, group), :] for e in range(2)]
            sendp[g, k] = jnp.concatenate(pieces, axis=0).astype(bf16)
            return carry

        lax.fori_loop(0, z.chips, other_rows, 0, unroll=16)
        sums_pair.append(pair_copy(2 + g, sendp.at[g], part.at[g]))
        sums_pair[g].start()

    def sums_copy(i, source):
        return pltpu.make_async_remote_copy(
            src_ref=send.at[peer_chip(i)], dst_ref=recv.at[source], send_sem=es_sem, recv_sem=er_sem,
            device_id={"ctx": peer_chip(i) * CORES + core}, device_id_type=MESH,
        )

    def stat_copy(i, source):
        return pltpu.make_async_remote_copy(
            src_ref=statf.at[peer_chip(i)], dst_ref=statr.at[source], send_sem=ss_sem, recv_sem=sr_sem,
            device_id={"ctx": peer_chip(i) * CORES + core}, device_id_type=MESH,
        )

    stat_pair.wait_recv()
    whole = jnp.where(lane_s < LANES // 2, stat[...], stat[...] + statp[...])
    for b in range(z.seqs):
        statf[b] = whole[b : b + 1]
    for i in order:
        stat_copy(i, chip).start()
    statr[chip] = statf[chip]
    for c in sums_pair:
        c.wait_recv()

    def own_rows(k, carry):
        halves = [part[g, k].astype(f32) for g in range(2)]
        theirs = jnp.concatenate([halves[g][e * group : (e + 1) * group] for e in range(2) for g in range(2)], axis=0)
        send[k] = (yt[pl.ds((k * CORES + core) * z.head_stride, z.heads), :] + theirs).astype(bf16)
        return carry

    lax.fori_loop(0, z.chips, own_rows, 0, unroll=16)

    for i in order:
        sums_copy(i, chip).start()
    recv[chip] = send[chip]

    all_stats = all_copies(z.chips - 1, statf, statr, ss_sem, sr_sem)
    all_sums = all_copies(z.chips - 1, send, recv, es_sem, er_sem)
    all_stats.wait_recv()

    s = jnp.concatenate([statr[d] for d in range(z.chips)], axis=0)
    s = jnp.where(core == 0, s, pltpu.roll(s, LANES - z.heads, 1))
    t = pltpu.roll(s, LANES // 2, 1)
    top = jnp.max(s, axis=0, keepdims=True)
    factor = jnp.exp(s - top)
    total = jnp.sum(factor * t, axis=0, keepdims=True)
    lane_d = lax.broadcasted_iota(jnp.int32, (z.chips, LANES), 1)
    share = jnp.where(lane_d < z.heads, factor / jnp.where(lane_d < z.heads, total, 1.0), 0.0)
    share = jnp.transpose(jnp.concatenate([share, jnp.zeros((LANES - z.chips, LANES), f32)], axis=0))
    shares[...] = share
    all_sums.wait_recv()
    merged = jnp.zeros((z.heads, z.value), f32)
    for d in range(z.chips):
        merged = merged + shares[0 : z.heads, d : d + 1] * recv[d].astype(f32)
    acc[...] = merged
    for h in range(z.heads):
        at = (h % 2) * z.pairs + h // 2
        row_out[:, h * z.value : (h + 1) * z.value] = acc[at : at + 1, :].astype(out_ref.dtype)
    out_copy = pltpu.make_async_copy(row_out, out_ref, out_sem)
    out_copy.start()

    def sent_hub():
        rows_hub.wait_send()
        forward(0).wait_send()
        forward(1).wait_send()

    pl.when(hub)(sent_hub)
    pl.when(jnp.logical_not(hub))(lambda: rows_leaf.wait_send())
    all_stats.wait_send()
    all_sums.wait_send()
    for c in (top_copy, stat_pair, *sums_pair):
        c.wait_send()
    out_copy.wait()


def per_device(
    query_nope, query_rope, cache_latent, cache_rope, key_up, value_up, lengths, block_owner, block_number,
):
    ctx = lax.axis_size("ctx")
    heads, nope, latent = key_up.shape
    slots, block, _ = cache_latent.shape
    z = Sizes(
        ctx, query_nope.shape[0] * ctx, heads, nope, query_rope.shape[1] // heads, latent, value_up.shape[2],
        slots, block, lengths.shape[0],
    )
    any_spec = pl.BlockSpec(memory_space=pl.ANY)
    V, S, D = pltpu.VMEM, pltpu.SMEM, pltpu.SemaphoreType.DMA
    span = z.rows * z.head_stride
    scratch = [
        V(query_nope.shape, bf16), V(query_rope.shape, bf16), V(cache_latent.shape, bf16), V(cache_rope.shape, bf16),
        V(key_up.shape, bf16), V(value_up.shape, bf16), S(lengths.shape, jnp.int32), S(block_owner.shape, jnp.int32),
        S(block_number.shape, jnp.int32), V((1, slots), jnp.int32), V((8, LANES), jnp.int32), S((8, LANES), jnp.int32),
        V((z.rows, z.block_rows, LANES), bf16),
        V((z.block_rows, LANES), bf16),
        V((z.block_rows, LANES), f32),
        V((z.rows * z.gather_stride, LANES), f32),
        V((slots, z.key_stride, LANES), f32),
        V((slots, latent, block), bf16),
        V((z.chunks * span, LANES), f32),
        V((z.seqs, z.queries, latent), bf16),
        V((z.seqs, z.queries, LANES), bf16),
        V((slots, z.queries, block), f32),
        V((slots, z.queries, block), f32),
        V((z.seqs, z.queries, block), f32),
        V((z.seqs, z.queries, block), f32),
        V((slots, z.queries, block), f32),
        V((slots, z.queries, latent), f32),
        V((z.chunks * span, LANES), f32),
        V((span, LANES), f32),
        V((2, z.chips, heads // 2, z.value), bf16),
        V((2, z.chips, heads // 2, z.value), bf16),
        V((z.chips, heads, z.value), bf16),
        V((z.chips, heads, z.value), bf16),
        V((z.seqs, LANES), f32),
        V((z.seqs, LANES), f32),
        V((z.seqs, 1, LANES), f32),
        V((z.chips, 1, LANES), f32),
        V((LANES, LANES), f32),
        V((heads, z.value), f32),
        V((1, heads * z.value), bf16),
        D,
        D((13,)), D, D, D((2,)), D((2,)), D((2,)),
        D((4,)), D((4,)),
        D, D, D, D,
    ]
    return pl.pallas_call(
        functools.partial(kernel, z),
        out_shape=jax.ShapeDtypeStruct((1, heads * z.value), bf16),
        in_specs=[any_spec] * 10,
        out_specs=any_spec,
        scratch_shapes=scratch,
        compiler_params=pltpu.CompilerParams(
            collective_id=0, has_side_effects=True, vmem_limit_bytes=64 * 1024 * 1024 - 65536
        ),
    )(
        query_nope, query_rope, cache_latent, cache_rope, key_up, value_up, lengths, block_owner,
        block_owner.reshape(1, slots), block_number,
    )


def solution(mesh):
    return jax.shard_map(
        per_device,
        mesh=mesh,
        in_specs=(
            P("ctx", "head"), P("ctx", "head"), P("ctx", None, None), P("ctx", None), P("head", None, None),
            P("head", None, None), P(), P("ctx"), P("ctx"),
        ),
        out_specs=P("ctx", "head"),
        check_vma=False,
    )
```
